32 devices in a mesh: data: 1 (over z), model: 4 (over y), time: 8 (over x, core).
Axes of the slice: x: 4, y: 4, z: 1, core: 2. Of those that a mesh axis runs over, the one named last changes fastest.
The devices are a block of a 4x4x8 slice.
Arguments:
- x_init: float32 [64, 16, 256], P('data')
- w_up: bfloat16 [256, 1152], P(None, 'model')
- w_down: bfloat16 [1152, 256], P('model')
- mod_scale: bfloat16 [128, 1152], P('time', 'model')
- mod_shift: bfloat16 [128, 1152], P('time', 'model')
- step_size: float32 [128], P('time')
Outputs:
- output: float32 [128, 64, 16, 256], P('time', 'data')
All inputs are finite; a program needn't handle non-finite values.
Results may differ from the reference program's by a relative error of at most 0.001.
Values are sent between devices in bfloat16 or wider.
A program may use at most 768 MiB of HBM per device.

```python
import jax
import jax.numpy as jnp
from jax import lax

STEPS = 128
BATCH = 64
TOKENS = 16
CHAN = 256
HIDDEN = 1152
SWEEPS = 4


def setup_inputs(seed: int = 0, part: int = 0) -> dict:
    base_key = jax.random.key(seed)
    key_list = jax.random.split(base_key, 6)
    part_key = jax.random.fold_in(key_list[5], part)
    x_init = jax.random.normal(part_key, (BATCH, TOKENS, CHAN), jnp.float32)
    w_up = (jax.random.normal(key_list[0], (CHAN, HIDDEN), jnp.float32) * CHAN ** -0.5).astype(jnp.bfloat16)
    w_down = (jax.random.normal(key_list[1], (HIDDEN, CHAN), jnp.float32) * HIDDEN ** -0.5).astype(jnp.bfloat16)
    mod_scale = (0.5 * jax.random.normal(key_list[2], (STEPS, HIDDEN), jnp.float32)).astype(jnp.bfloat16)
    mod_shift = (0.5 * jax.random.normal(key_list[3], (STEPS, HIDDEN), jnp.float32)).astype(jnp.bfloat16)
    step_size = (3.0 / STEPS) * jax.random.uniform(key_list[4], (STEPS,), jnp.float32, 0.2, 1.8)
    return {'x_init': x_init, 'w_up': w_up, 'w_down': w_down, 'mod_scale': mod_scale, 'mod_shift': mod_shift, 'step_size': step_size}


def drift_at(latent, scale_row, shift_row, step_val, w_up, w_down):
    flat_lat = latent.reshape(BATCH * TOKENS, CHAN).astype(jnp.bfloat16)
    pre_act = jnp.dot(flat_lat, w_up, preferred_element_type=jnp.float32)
    hidden = jax.nn.gelu(pre_act * (1.0 + scale_row.astype(jnp.float32)) + shift_row.astype(jnp.float32), approximate=True)
    proj_out = jnp.dot(hidden.astype(jnp.bfloat16), w_down, preferred_element_type=jnp.float32)
    return step_val * proj_out.reshape(BATCH, TOKENS, CHAN)


def reference(x_init, w_up, w_down, mod_scale, mod_shift, step_size):
    def drift_step(packed):
        return drift_at(packed[0], packed[1], packed[2], packed[3], w_up, w_down)

    def one_sweep(latents, unused):
        drifts = lax.map(drift_step, (latents, mod_scale, mod_shift, step_size))
        prefix = jnp.cumsum(drifts, axis=0) - drifts
        return x_init[None] + prefix, unused

    start_lat = jnp.broadcast_to(x_init[None], (STEPS, BATCH, TOKENS, CHAN))
    final_lat, unused = lax.scan(one_sweep, start_lat, None, length=SWEEPS)
    return final_lat
```

```python
import functools
import math

import jax
import jax.numpy as jnp
from jax import lax
from jax.experimental import pallas as pl
from jax.experimental.pallas import tpu as pltpu
from jax.sharding import PartitionSpec as P

SWEEPS = 4
ROWS = 16
STAGES = 4
F32, BF16 = jnp.float32, jnp.bfloat16
MESH_ID = pl.DeviceIdType.MESH
ROOT = math.sqrt(2.0 / math.pi)


def kernel(n_t, n_m, h_ref, x0_ref, w1_ref, w2_ref, sc_ref, sh_ref, out_ref, xbuf, obuf, rbuf, robuf, gbuf, stage,
           s1s, s1r, s2s, s2r, s3s, s3r, o1s, o1r, o2s, o2r, o3s, o3r, out_sem):
    me_t = lax.axis_index('time')
    me_m = lax.axis_index('model')
    n_k = xbuf.shape[0]
    span = xbuf.shape[2] // ROWS
    half = xbuf.shape[2] // 2
    hid = w1_ref.shape[1]
    n_x = n_t // 2
    up, down = lax.rem(me_m + 1, n_m), lax.rem(me_m + n_m - 1, n_m)
    chunks = [(lo, min(lo + 256, hid)) for lo in range(0, hid, 256)]

    def peer(q, sign):
        qx, dc = q // 2, q % 2
        dx = qx + (qx // 2) * (5 - 2 * qx)
        return ((me_t // 2 + n_x + sign * dx) % n_x) * 2 + (me_t % 2 + dc) % 2

    def remote(src, dst, send, recv, **where):
        return pltpu.make_async_remote_copy(src_ref=src, dst_ref=dst, send_sem=send, recv_sem=recv, device_id=where, device_id_type=MESH_ID)

    def drift(x, tb, same):
        for lo, hi in chunks:
            p = jnp.dot(x, w1_ref[:, lo:hi], preferred_element_type=F32)
            for j in range(span):
                pj = p if same else p[j * ROWS:(j + 1) * ROWS]
                v = pj * sc_ref[tb, j:j + 1, lo:hi] + sh_ref[tb, j:j + 1, lo:hi]
                t = jnp.tanh(v * (2 * ROOT + (8 * 0.044715 * ROOT) * (v * v)))
                gbuf[j * ROWS:(j + 1) * ROWS, lo:hi] = (v + v * t).astype(BF16)
        return jnp.dot(gbuf[...], w2_ref[...], preferred_element_type=F32)

    def sweep(k, number):
        x0 = x0_ref[pl.ds(((me_m * n_t + me_t) * n_k + k) * ROWS, ROWS), :]

        def body(tb, acc):
            if number == 0:
                f = drift(x0.astype(BF16), tb, True)
            else:
                f = drift(xbuf[k, tb], tb, False)
            if number == SWEEPS - 1:
                obuf[k, tb] = acc
            for j in range(span):
                if number < SWEEPS - 1:
                    xbuf[k, tb, j * ROWS:(j + 1) * ROWS, :] = (x0 + acc).astype(BF16)
                acc = acc + h_ref[tb * span + j] * f[j * ROWS:(j + 1) * ROWS]
            return acc

        lax.fori_loop(0, n_t, body, jnp.zeros_like(x0))

    def x_send(k):
        @pl.loop(1, n_t)
        def _(q):
            to = peer(q, 1)
            remote(xbuf.at[k, to], rbuf.at[0, k, me_t], s1s.at[k, q], s1r.at[k, q], time=to).start()
        rbuf[0, k, me_t] = xbuf[k, me_t]

    def x_row(q, k):
        src = peer(q, -1)

        @pl.when(q > 0)
        def _():
            remote(xbuf.at[k, 0], rbuf.at[0, k, src], s1s.at[k, q], s1r.at[k, q], time=src).wait_recv()
        i = k * n_t + q
        remote(rbuf.at[0, k, src], rbuf.at[1, k, src], s2s.at[0, i], s2r.at[0, i], model=up).start()
        remote(rbuf.at[0, k, src], rbuf.at[2, k, src], s2s.at[1, i], s2r.at[1, i], model=down).start()

    def x_pass(q, k):
        src = peer(q, -1)
        i = k * n_t + q
        for d, to in ((0, up), (1, down)):
            remote(rbuf.at[0, k, src], rbuf.at[1 + d, k, src], s2s.at[d, i], s2r.at[d, i], model=to).wait_recv()
            part = pl.ds(d * half, half)
            remote(rbuf.at[1 + d, k, src, part], rbuf.at[3, k, src, part], s3s.at[d, i], s3r.at[d, i], model=to).start()

    def x_far(q, k):
        src = peer(q, -1)
        i = k * n_t + q
        for d, to in ((0, up), (1, down)):
            part = pl.ds(d * half, half)
            remote(rbuf.at[1 + d, k, src, part], rbuf.at[3, k, src, part], s3s.at[d, i], s3r.at[d, i], model=to).wait_recv()

    def o_send(k):
        @pl.loop(1, n_t)
        def _(q):
            to = peer(q, 1)
            remote(obuf.at[k, to], robuf.at[0, k, me_t], o1s.at[k, q], o1r.at[k, q], time=to).start()
        robuf[0, k, me_t] = obuf[k, me_t]

    def o_row(k):
        @pl.loop(1, n_t)
        def _(q):
            src = peer(q, -1)
            remote(obuf.at[k, 0], robuf.at[0, k, src], o1s.at[k, q], o1r.at[k, q], time=src).wait_recv()
        remote(robuf.at[0, k], robuf.at[1, k], o2s.at[0, k], o2r.at[0, k], model=up).start()
        remote(robuf.at[0, k], robuf.at[2, k], o2s.at[1, k], o2r.at[1, k], model=down).start()

    def o_pass(k):
        for d, to in ((0, up), (1, down)):
            remote(robuf.at[0, k], robuf.at[1 + d, k], o2s.at[d, k], o2r.at[d, k], model=to).wait_recv()
            part = pl.ds(d * n_x, n_x)
            remote(robuf.at[1 + d, k, part], robuf.at[3, k, part], o3s.at[d, k], o3r.at[d, k], model=to).start()

    def o_far(k):
        for d, to in ((0, up), (1, down)):
            part = pl.ds(d * n_x, n_x)
            remote(robuf.at[1 + d, k, part], robuf.at[3, k, part], o3s.at[d, k], o3r.at[d, k], model=to).wait_recv()

    def out_copy(slot, row):
        return pltpu.make_async_copy(stage.at[slot], out_ref.at[:, pl.ds(row, ROWS), :], out_sem.at[slot])

    def finish(rel, q, k, number):
        src = peer(q, -1)
        origin = (me_m + (n_m - rel) + (rel // 2) * (2 * rel - 5)) % n_m
        row = ((origin * n_t + src) * n_k + k) * ROWS
        slot = number % STAGES

        @pl.when(number >= STAGES)
        def _():
            out_copy(slot, 0).wait()
        f = drift(rbuf[rel, k, src], me_t, False)
        x0 = x0_ref[pl.ds(row, ROWS), :]
        acc = robuf[rel, k, src]
        for j in range(span):
            stage[slot, j] = x0 + acc
            acc = acc + h_ref[me_t * span + j] * f[j * ROWS:(j + 1) * ROWS]
        out_copy(slot, row).start()

    barrier = pltpu.get_barrier_semaphore()

    @pl.loop(1, n_t)
    def _(q):
        pl.semaphore_signal(barrier, inc=1, device_id={'time': peer(q, 1)}, device_id_type=MESH_ID)
    for to in (up, down):
        pl.semaphore_signal(barrier, inc=1, device_id={'model': to}, device_id_type=MESH_ID)
    pl.semaphore_wait(barrier, n_t + 1)

    for number in range(SWEEPS - 1):
        sweep(0, number)
    x_send(0)
    x_row(0, 0)
    sweep(0, SWEEPS - 1)
    o_send(0)
    x_row(1, 0)
    sweep(1, 0)
    x_row(2, 0)
    x_row(3, 0)
    x_pass(0, 0)
    sweep(1, 1)
    x_row(4, 0)
    x_row(5, 0)
    x_pass(1, 0)
    o_row(0)
    sweep(1, 2)
    x_send(1)
    x_row(6, 0)
    x_row(7, 0)
    x_pass(2, 0)
    o_pass(0)
    sweep(1, SWEEPS - 1)
    o_send(1)
    x_pass(3, 0)
    o_far(0)

    early = 4

    @pl.loop(0, n_k * n_t)
    def _(i):
        k, q = i // n_t, i % n_t

        @pl.when(i >= early)
        def _():
            x_pass(q, k)

        @pl.when(i < n_t)
        def _():
            x_row(q, 1)

        @pl.when(i == 2)
        def _():
            o_row(1)

        @pl.when(i == 5)
        def _():
            o_pass(1)

        @pl.when(i == n_t)
        def _():
            o_far(1)

        @pl.loop(0, n_m)
        def _(rel):
            @pl.when(rel == n_m - 1)
            def _():
                x_far(q, k)
            finish(rel, q, k, i * n_m + rel)

    for slot in range(STAGES):
        out_copy(slot, 0).wait()

    @pl.loop(0, n_k * n_t)
    def _(i):
        k, q = i // n_t, i % n_t

        @pl.when(q > 0)
        def _():
            remote(xbuf.at[k, 0], rbuf.at[0, k, 0], s1s.at[k, q], s1r.at[k, q], time=peer(q, 1)).wait_send()
            remote(obuf.at[k, 0], robuf.at[0, k, 0], o1s.at[k, q], o1r.at[k, q], time=peer(q, 1)).wait_send()
        for d, to in ((0, up), (1, down)):
            part = pl.ds(d * half, half)
            remote(rbuf.at[0, k, 0], rbuf.at[1 + d, k, 0], s2s.at[d, i], s2r.at[d, i], model=to).wait_send()
            remote(rbuf.at[1 + d, k, 0, part], rbuf.at[3, k, 0, part], s3s.at[d, i], s3r.at[d, i], model=to).wait_send()
    for k in range(n_k):
        for d, to in ((0, up), (1, down)):
            part = pl.ds(d * n_x, n_x)
            remote(robuf.at[0, k], robuf.at[1 + d, k], o2s.at[d, k], o2r.at[d, k], model=to).wait_send()
            remote(robuf.at[1 + d, k, part], robuf.at[3, k, part], o3s.at[d, k], o3r.at[d, k], model=to).wait_send()


def solution(mesh):
    n_t, n_m = mesh.shape['time'], mesh.shape['model']

    def device_body(x_init, w_up, w_down, mod_scale, mod_shift, step_size):
        span, chan = mod_scale.shape[0], x_init.shape[-1]
        rows = x_init.shape[0] * x_init.shape[1]
        w1 = lax.all_gather(w_up, 'model', axis=1, tiled=True)
        w2 = lax.all_gather(w_down, 'model', axis=0, tiled=True)
        mods = jnp.stack([mod_scale, mod_shift])
        mods = lax.all_gather(lax.all_gather(mods, 'model', axis=2, tiled=True), 'time', axis=1, tiled=True).astype(F32)
        mods = mods.reshape(2, n_t, span, -1)
        scale, shift = 0.5 * (1.0 + mods[0]), 0.5 * mods[1]
        steps = lax.all_gather(step_size, 'time', axis=0, tiled=True)
        hid = w1.shape[1]
        n_k = rows // (n_t * n_m * ROWS)
        vmem = pl.BlockSpec(memory_space=pltpu.VMEM)
        sem = lambda *shape: pltpu.SemaphoreType.DMA(shape)
        out = pl.pallas_call(
            functools.partial(kernel, n_t, n_m),
            out_shape=jax.ShapeDtypeStruct((span, rows, chan), F32),
            in_specs=[pl.BlockSpec(memory_space=pltpu.SMEM)] + [vmem] * 5,
            out_specs=pl.BlockSpec(memory_space=pl.ANY),
            scratch_shapes=[
                pltpu.VMEM((n_k, n_t, span * ROWS, chan), BF16),
                pltpu.VMEM((n_k, n_t, ROWS, chan), F32),
                pltpu.VMEM((n_m, n_k, n_t, span * ROWS, chan), BF16),
                pltpu.VMEM((n_m, n_k, n_t, ROWS, chan), F32),
                pltpu.VMEM((span * ROWS, hid), BF16),
                pltpu.VMEM((STAGES, span, ROWS, chan), F32),
                sem(n_k, n_t), sem(n_k, n_t),
                sem(2, n_k * n_t), sem(2, n_k * n_t), sem(2, n_k * n_t), sem(2, n_k * n_t),
                sem(n_k, n_t), sem(n_k, n_t),
                sem(2, n_k), sem(2, n_k), sem(2, n_k), sem(2, n_k),
                sem(STAGES),
            ],
            compiler_params=pltpu.CompilerParams(collective_id=0, has_side_effects=True, vmem_limit_bytes=48 << 20),
        )(steps, x_init.reshape(rows, chan), w1, w2, scale, shift)
        return out.reshape((span,) + x_init.shape)

    return jax.shard_map(device_body, mesh=mesh, in_specs=(P('data', None, None), P(None, 'model'), P('model', None), P('time', 'model'), P('time', 'model'), P('time')), out_specs=P('time', 'data', None, None), check_vma=False)
```

```python
import functools
import math

import jax
import jax.numpy as jnp
from jax import lax
from jax.experimental import pallas as pl
from jax.experimental.pallas import tpu as pltpu
from jax.sharding import PartitionSpec as P

SWEEPS = 4
ROWS = 16
STAGES = 4
F32, BF16 = jnp.float32, jnp.bfloat16
MESH_ID = pl.DeviceIdType.MESH
ROOT = math.sqrt(2.0 / math.pi)


def kernel(n_t, n_m, h_ref, x0_ref, wu_ref, wd_ref, ms_ref, mb_ref, out_ref, w1_ref, w2_ref, w1raw, w2raw, modraw, modall, hall, sc_ref, sh_ref,
           xbuf, obuf, rbuf, robuf, gbuf, stage, gws, gwr, gfs, gfr, gds, gdr, ms, mr, mxs, mxr, mds, mdr, hs, hr,
           s1s, s1r, s2s, s2r, s3s, s3r, o1s, o1r, o2s, o2r, o3s, o3r, out_sem):
    me_t = lax.axis_index('time')
    me_m = lax.axis_index('model')
    me_x, me_c = me_t // 2, me_t % 2
    n_k, n_x = xbuf.shape[0], n_t // 2
    block = xbuf.shape[2] // 2
    span = block // ROWS
    half = block // 2
    hid_dev = wu_ref.shape[1]
    hid = n_m * hid_dev
    main = hid_dev // 128 * 128
    tail = hid_dev - main
    chunks = [(lo, min(lo + 256, hid)) for lo in range(0, hid, 256)]
    up, down, far = (me_m + 1) % n_m, (me_m + n_m - 1) % n_m, (me_m + 2) % n_m
    mate = me_x * 2 + (me_c + 1) % 2
    lanes = ((0, up), (1, down))

    def hop(qx):
        return qx + (qx // 2) * (5 - 2 * qx)

    def peer(q, sign):
        return ((me_x + n_x + sign * hop(q // 2)) % n_x) * 2 + (me_c + q % 2) % 2

    def remote(src, dst, send, recv, **where):
        return pltpu.make_async_remote_copy(src_ref=src, dst_ref=dst, send_sem=send, recv_sem=recv, device_id=where, device_id_type=MESH_ID)

    tables = ((wu_ref, w1raw), (wd_ref, w2raw))

    def w_part(ref, c):
        return pl.ds(c * (ref.shape[-2] // 2), ref.shape[-2] // 2)

    def w_first(i, d, to):
        own, raw = tables[i]
        return remote(own.at[w_part(own, me_c)], raw.at[me_m, w_part(own, me_c)], gws.at[i, d], gwr.at[i, d], model=to)

    def w_forward(d, to):
        own, raw = tables[d]
        origin = (down, up)[d]
        piece = raw.at[origin, w_part(own, me_c)]
        return remote(piece, piece, gfs.at[d], gfr.at[d], model=to)

    def w_share(i, place):
        own, raw = tables[i]
        piece = raw.at[(down, up, far)[place], w_part(own, me_c)]
        return remote(piece, piece, gds.at[i, place], gdr.at[i, place], time=mate)

    def mod_first(i, place):
        return remote((ms_ref, mb_ref)[i], modraw.at[i, me_m], ms.at[i, place], mr.at[i, place], model=(up, down, far)[place])

    def mod_time(qx):
        return remote(modall.at[me_t], modall.at[me_t], mxs.at[qx], mxr.at[qx], time=((me_x + hop(qx)) % n_x) * 2 + me_c)

    def mod_share(qx):
        row = ((me_x + n_x - hop(qx)) % n_x) * 2 + me_c
        return remote(modall.at[row], modall.at[row], mds.at[qx], mdr.at[qx], time=mate)

    def h_time(q):
        return remote(hall.at[me_t], hall.at[me_t], hs.at[q], hr.at[q], time=peer(q, 1))

    barrier = pltpu.get_barrier_semaphore()

    @pl.loop(1, n_t)
    def _(q):
        pl.semaphore_signal(barrier, inc=1, device_id={'time': peer(q, 1)}, device_id_type=MESH_ID)
    for to in (up, down, far):
        pl.semaphore_signal(barrier, inc=1, device_id={'model': to}, device_id_type=MESH_ID)
    for j in range(span):
        hall[me_t, j:j + 1, :] = jnp.full((1, hall.shape[2]), h_ref[j], F32)
    w1raw[me_m] = wu_ref[...]
    w2raw[me_m] = wd_ref[...]
    modraw[0, me_m] = ms_ref[...]
    modraw[1, me_m] = mb_ref[...]
    pl.semaphore_wait(barrier, n_t + 2)

    for place in range(3):
        for i in range(2):
            mod_first(i, place).start()
    for d, to in lanes:
        for i in range(2):
            w_first(i, d, to).start()

    @pl.loop(1, n_t)
    def _(q):
        h_time(q).start()

    def joined(pieces):
        return jnp.concatenate([p[:, :main] for p in pieces] + [jnp.concatenate([p[:, main:] for p in pieces], axis=1)], axis=1)

    for place in range(3):
        for i in range(2):
            mod_first(i, place).wait_recv()
    for i in range(2):
        modall[me_t, i] = joined([modraw[i, m].astype(F32) for m in range(n_m)]).astype(BF16)
    for qx in (1, 2, 3):
        mod_time(qx).start()
    mod_share(0).start()

    for d, to in lanes:
        for i in range(2):
            w_first(i, d, to).wait_recv()
        w_forward(d, to).start()
        for i in range(2):
            w_share(i, d).start()
    for qx in (1, 2, 3):
        mod_time(qx).wait_recv()
        mod_share(qx).start()
    for d, to in lanes:
        w_forward(d, to).wait_recv()
        w_share(d, 2).start()

    @pl.loop(1, n_t)
    def _(q):
        h_time(q).wait_recv()
    for place in range(3):
        for i in range(2):
            w_share(i, place).wait_recv()
    for qx in range(n_x):
        mod_share(qx).wait_recv()
    for m in range(n_m):
        w1_ref[:, m * main:(m + 1) * main] = w1raw[m][:, :main]
        w2_ref[m * main:(m + 1) * main, :] = w2raw[m, :main, :]
        w2_ref[n_m * main + m * tail:n_m * main + (m + 1) * tail, :] = w2raw[m, main:, :]
    w1_ref[:, n_m * main:] = jnp.concatenate([w1raw[m][:, main:].astype(F32) for m in range(n_m)], axis=1).astype(BF16)

    @pl.loop(0, n_t)
    def _(t):
        sc_ref[t] = 0.5 * (1.0 + modall[t, 0].astype(F32))
        sh_ref[t] = 0.5 * modall[t, 1].astype(F32)

    def drift(x, blocks, same):
        for lo, hi in chunks:
            p = jnp.dot(x, w1_ref[:, lo:hi], preferred_element_type=F32)
            for b, tb in enumerate(blocks):
                for j in range(span):
                    at = (b * span + j) * ROWS
                    v = (p if same else p[at:at + ROWS]) * sc_ref[tb, j:j + 1, lo:hi] + sh_ref[tb, j:j + 1, lo:hi]
                    t = jnp.tanh(v * (2 * ROOT + (8 * 0.044715 * ROOT) * (v * v)))
                    gbuf[at:at + ROWS, lo:hi] = (v + v * t).astype(BF16)
        return jnp.dot(gbuf[...], w2_ref[...], preferred_element_type=F32)

    def scaled(f, b, tb, j):
        at = (b * span + j) * ROWS
        h = hall[tb, j:j + 1, :]
        return f[at:at + ROWS] * jnp.concatenate([h] * (f.shape[1] // h.shape[1]), axis=1)

    def sweep(k, number):
        x0 = x0_ref[pl.ds(((k * n_m + me_m) * n_t + me_t) * ROWS, ROWS), :]

        def body(bx, acc):
            f = drift(x0.astype(BF16) if number == 0 else xbuf[k, bx], (2 * bx, 2 * bx + 1), number == 0)
            for b in range(2):
                if number == SWEEPS - 1:
                    obuf[k, 2 * bx + b] = acc
                for j in range(span):
                    if number < SWEEPS - 1:
                        at = (b * span + j) * ROWS
                        xbuf[k, bx, at:at + ROWS, :] = (x0 + acc).astype(BF16)
                    acc = acc + scaled(f, b, 2 * bx + b, j)
            return acc

        lax.fori_loop(0, n_x, body, jnp.zeros_like(x0))

    def sub(c):
        return pl.ds(c * block, block)

    def x_copy(k, q, to, src):
        return remote(xbuf.at[k, to // 2, sub(to % 2)], rbuf.at[0, k, src // 2, sub(src % 2)], s1s.at[k, q], s1r.at[k, q], time=to)

    def x_send(k):
        @pl.loop(1, n_t)
        def _(q):
            x_copy(k, q, peer(q, 1), me_t).start()
        rbuf[0, k, me_x, sub(me_c), :] = xbuf[k, me_x, sub(me_c), :]

    def x_ring(q, k, d, to):
        src = peer(q, -1)
        i = k * n_t + q
        return remote(rbuf.at[0, k, src // 2, sub(src % 2)], rbuf.at[1 + d, k, src // 2, sub(src % 2)], s2s.at[d, i], s2r.at[d, i], model=to)

    def x_next(q, k, d, to):
        src = peer(q, -1)
        i = k * n_t + q
        part = pl.ds((src % 2) * block + d * half, half)
        return remote(rbuf.at[1 + d, k, src // 2, part], rbuf.at[3, k, src // 2, part], s3s.at[d, i], s3r.at[d, i], model=to)

    def x_row(q, k):
        @pl.when(q > 0)
        def _():
            x_copy(k, q, me_t, peer(q, -1)).wait_recv()
        for d, to in lanes:
            x_ring(q, k, d, to).start()

    def x_pass(q, k):
        for d, to in lanes:
            x_ring(q, k, d, to).wait_recv()
            x_next(q, k, d, to).start()

    def x_far(q, k):
        for d, to in lanes:
            x_next(q, k, d, to).wait_recv()

    def o_copy(k, q, to, src):
        return remote(obuf.at[k, to], robuf.at[0, k, src], o1s.at[k, q], o1r.at[k, q], time=to)

    def o_ring(k, d, to):
        return remote(robuf.at[0, k], robuf.at[1 + d, k], o2s.at[d, k], o2r.at[d, k], model=to)

    def o_next(k, d, to):
        part = pl.ds(d * n_x, n_x)
        return remote(robuf.at[1 + d, k, part], robuf.at[3, k, part], o3s.at[d, k], o3r.at[d, k], model=to)

    def o_send(k):
        @pl.loop(1, n_t)
        def _(q):
            o_copy(k, q, peer(q, 1), me_t).start()
        robuf[0, k, me_t] = obuf[k, me_t]

    def o_row(k):
        @pl.loop(1, n_t)
        def _(q):
            o_copy(k, q, me_t, peer(q, -1)).wait_recv()
        for d, to in lanes:
            o_ring(k, d, to).start()

    def o_pass(k):
        for d, to in lanes:
            o_ring(k, d, to).wait_recv()
            o_next(k, d, to).start()

    def o_far(k):
        for d, to in lanes:
            o_next(k, d, to).wait_recv()

    def out_copy(slot, row):
        return pltpu.make_async_copy(stage.at[slot], out_ref.at[:, pl.ds(row, 2 * ROWS), :], out_sem.at[slot])

    def finish(rel, pair, number):
        k, src = pair // n_x, (me_x + n_x - hop(pair % n_x)) % n_x
        origin = (me_m + (n_m - rel) + (rel // 2) * (2 * rel - 5)) % n_m
        row = (((k * n_m + origin) * n_x + src) * 2) * ROWS
        slot = number % STAGES

        @pl.when(number >= STAGES)
        def _():
            out_copy(slot, 0).wait()
        f = drift(rbuf[rel, k, src], (me_t, me_t), False)
        for b in range(2):
            x0 = x0_ref[pl.ds(row + b * ROWS, ROWS), :]
            acc = robuf[rel, k, 2 * src + b]
            for j in range(span):
                stage[slot, j, b * ROWS:(b + 1) * ROWS, :] = x0 + acc
                acc = acc + scaled(f, b, me_t, j)
        out_copy(slot, row).start()

    @pl.loop(0, n_k * SWEEPS)
    def _(step):
        k, number = step // SWEEPS, step % SWEEPS

        @pl.when(number == 0)
        def _():
            sweep(k, 0)

        @pl.when(number % (SWEEPS - 1) > 0)
        def _():
            sweep(k, 1)

        @pl.when(number == SWEEPS - 2)
        def _():
            x_send(k)

        @pl.when(number == SWEEPS - 1)
        def _():
            sweep(k, SWEEPS - 1)
            o_send(k)

        @pl.when(step == SWEEPS - 2)
        def _():
            x_row(0, 0)

        @pl.when(step == SWEEPS - 1)
        def _():
            x_row(1, 0)

        @pl.when(step == SWEEPS)
        def _():
            x_pass(0, 0)
            x_row(2, 0)
            x_row(3, 0)

        @pl.when(step == SWEEPS + 1)
        def _():
            x_pass(1, 0)
            o_row(0)
            x_row(4, 0)
            x_row(5, 0)

        @pl.when(step == SWEEPS + 2)
        def _():
            x_pass(2, 0)
            x_pass(3, 0)
            o_pass(0)

    o_far(0)

    pairs = n_k * n_x
    early, ahead = 2, 3
    for c in range(2):
        x_row(ahead % n_x * 2 + c, ahead // n_x)

    @pl.loop(0, n_m * pairs)
    def _(n):
        p, turn = (n + 1) // n_m, (n + 1) % n_m
        rel, pair = (turn + n_m - 1) % n_m, p - (n_m - turn) // n_m

        @pl.when(turn == 0)
        def _():
            @pl.when(p < pairs)
            def _():
                @pl.when(p >= early)
                def _():
                    for c in range(2):
                        x_pass(p % n_x * 2 + c, p // n_x)

            @pl.when(p < pairs - ahead)
            def _():
                for c in range(2):
                    x_row((p + ahead) % n_x * 2 + c, (p + ahead) // n_x)

            @pl.when(p == 1)
            def _():
                o_row(1)

            @pl.when(p == 3)
            def _():
                o_pass(1)

            @pl.when(p == n_x)
            def _():
                o_far(1)

            for c in range(2):
                x_far(pair % n_x * 2 + c, pair // n_x)
        finish(rel, pair, n)

    for slot in range(STAGES):
        out_copy(slot, 0).wait()

    for d, to in lanes:
        for i in range(2):
            w_first(i, d, to).wait_send()
        w_forward(d, to).wait_send()
    for place in range(3):
        for i in range(2):
            w_share(i, place).wait_send()
            mod_first(i, place).wait_send()
    for qx in range(n_x):
        if qx:
            mod_time(qx).wait_send()
        mod_share(qx).wait_send()

    @pl.loop(1, n_t)
    def _(q):
        h_time(q).wait_send()

    @pl.loop(0, n_k * n_t)
    def _(i):
        k, q = i // n_t, i % n_t

        @pl.when(q > 0)
        def _():
            x_copy(k, q, peer(q, 1), me_t).wait_send()
            o_copy(k, q, peer(q, 1), me_t).wait_send()
        for d, to in lanes:
            x_ring(q, k, d, to).wait_send()
            x_next(q, k, d, to).wait_send()
    for k in range(n_k):
        for d, to in lanes:
            o_ring(k, d, to).wait_send()
            o_next(k, d, to).wait_send()


def solution(mesh):
    n_t, n_m = mesh.shape['time'], mesh.shape['model']

    def device_body(x_init, w_up, w_down, mod_scale, mod_shift, step_size):
        (span, hid_dev), chan = mod_scale.shape, x_init.shape[-1]
        rows = x_init.shape[0] * x_init.shape[1]
        hid = n_m * hid_dev
        n_k, n_x = rows // (n_t * n_m * ROWS), n_t // 2
        vmem = pl.BlockSpec(memory_space=pltpu.VMEM)
        sem = lambda *shape: pltpu.SemaphoreType.DMA(shape)
        out = pl.pallas_call(
            functools.partial(kernel, n_t, n_m),
            out_shape=jax.ShapeDtypeStruct((span, rows, chan), F32),
            in_specs=[pl.BlockSpec(memory_space=pltpu.SMEM)] + [vmem] * 5,
            out_specs=pl.BlockSpec(memory_space=pl.ANY),
            scratch_shapes=[
                pltpu.VMEM((chan, hid), BF16),
                pltpu.VMEM((hid, chan), BF16),
                pltpu.VMEM((n_m, chan, hid_dev), BF16),
                pltpu.VMEM((n_m, hid_dev, chan), BF16),
                pltpu.VMEM((2, n_m, span, hid_dev), BF16),
                pltpu.VMEM((n_t, 2, span, hid), BF16),
                pltpu.VMEM((n_t, span, 128), F32),
                pltpu.VMEM((n_t, span, hid), F32),
                pltpu.VMEM((n_t, span, hid), F32),
                pltpu.VMEM((n_k, n_x, 2 * span * ROWS, chan), BF16),
                pltpu.VMEM((n_k, n_t, ROWS, chan), F32),
                pltpu.VMEM((n_m, n_k, n_x, 2 * span * ROWS, chan), BF16),
                pltpu.VMEM((n_m, n_k, n_t, ROWS, chan), F32),
                pltpu.VMEM((2 * span * ROWS, hid), BF16),
                pltpu.VMEM((STAGES, span, 2 * ROWS, chan), F32),
                sem(2, 2), sem(2, 2), sem(2), sem(2), sem(2, 3), sem(2, 3),
                sem(2, 3), sem(2, 3), sem(n_x), sem(n_x), sem(n_x), sem(n_x), sem(n_t), sem(n_t),
                sem(n_k, n_t), sem(n_k, n_t),
                sem(2, n_k * n_t), sem(2, n_k * n_t), sem(2, n_k * n_t), sem(2, n_k * n_t),
                sem(n_k, n_t), sem(n_k, n_t),
                sem(2, n_k), sem(2, n_k), sem(2, n_k), sem(2, n_k),
                sem(STAGES),
            ],
            compiler_params=pltpu.CompilerParams(collective_id=0, has_side_effects=True, vmem_limit_bytes=48 << 20),
        )(step_size, x_init.reshape(rows, chan), w_up, w_down, mod_scale, mod_shift)
        return out.reshape((span,) + x_init.shape)

    return jax.shard_map(device_body, mesh=mesh, in_specs=(P('data', None, None), P(None, 'model'), P('model', None), P('time', 'model'), P('time', 'model'), P('time')), out_specs=P('time', 'data', None, None), check_vma=False)
```

```python
import functools
import math

import jax
import jax.numpy as jnp
from jax import lax
from jax.experimental import pallas as pl
from jax.experimental.pallas import tpu as pltpu
from jax.sharding import PartitionSpec as P

SWEEPS = 4
VMEM_BYTES = 67043328
ROWS = 16
STAGES = 4
F32, BF16 = jnp.float32, jnp.bfloat16
MESH_ID = pl.DeviceIdType.MESH
ROOT = math.sqrt(2.0 / math.pi)


def kernel(n_t, n_m, h_hbm, x0_hbm, wu_hbm, wd_hbm, ms_hbm, mb_hbm, out_ref, h_ref, x0_ref, w1_ref, w1t_ref, w2_ref, modraw, modall, hall, sc_ref, sh_ref,
           xbuf, obuf, rbuf, robuf, gbuf, own_sem, gws, gwr, gfs, gfr, gds, gdr, ms, mr, mxs, mxr, mds, mdr, hs, hr,
           s1s, s1r, s2s, s2r, s3s, s3r, o1s, o1r, o2s, o2r, o3s, o3r):
    me_t = lax.axis_index('time')
    me_m = lax.axis_index('model')
    me_x, me_c = me_t // 2, me_t % 2
    n_k, n_x = xbuf.shape[0], n_t // 2
    block = xbuf.shape[2] // 2
    span = block // ROWS
    half = block // 2
    hid_dev = modraw.shape[3]
    hid = n_m * hid_dev
    chunks = [(lo, min(lo + 256, hid)) for lo in range(0, hid, 256)]
    up, down, far = (me_m + 1) % n_m, (me_m + n_m - 1) % n_m, (me_m + 2) % n_m
    mate = me_x * 2 + (me_c + 1) % 2
    lanes = ((0, up), (1, down))

    def hop(qx):
        return qx + (qx // 2) * (5 - 2 * qx)

    def peer(q, sign):
        return ((me_x + n_x + sign * hop(q // 2)) % n_x) * 2 + (me_c + q % 2) % 2

    def remote(src, dst, send, recv, **where):
        return pltpu.make_async_remote_copy(src_ref=src, dst_ref=dst, send_sem=send, recv_sem=recv, device_id=where, device_id_type=MESH_ID)

    tables = (w1t_ref, w2_ref)

    def w_rows(origin, c):
        rows = hid_dev // 2
        return pl.ds(pl.multiple_of(origin * hid_dev + c * rows, 16), rows)

    def w_first(i, d, to):
        piece = tables[i].at[w_rows(me_m, me_c)]
        return remote(piece, piece, gws.at[i, d], gwr.at[i, d], model=to)

    def w_forward(d, to):
        piece = tables[d].at[w_rows((down, up)[d], me_c)]
        return remote(piece, piece, gfs.at[d], gfr.at[d], model=to)

    def w_share(i, place):
        piece = tables[i].at[w_rows((down, up, far)[place], me_c)]
        return remote(piece, piece, gds.at[i, place], gdr.at[i, place], time=mate)

    def mod_first(i, place):
        return remote(modraw.at[i, me_m], modraw.at[i, me_m], ms.at[i, place], mr.at[i, place], model=(up, down, far)[place])

    def mod_time(qx):
        return remote(modall.at[me_t], modall.at[me_t], mxs.at[qx], mxr.at[qx], time=((me_x + hop(qx)) % n_x) * 2 + me_c)

    def mod_share(qx):
        row = ((me_x + n_x - hop(qx)) % n_x) * 2 + me_c
        return remote(modall.at[row], modall.at[row], mds.at[qx], mdr.at[qx], time=mate)

    def h_time(q):
        return remote(hall.at[me_t], hall.at[me_t], hs.at[q], hr.at[q], time=peer(q, 1))

    mine = pl.ds(pl.multiple_of(me_m * hid_dev, 16), hid_dev)
    own = [pltpu.make_async_copy(src, dst, own_sem.at[i]) for i, (src, dst) in enumerate((
        (ms_hbm, modraw.at[0, me_m]), (mb_hbm, modraw.at[1, me_m]), (wu_hbm, w1t_ref.at[mine]), (wd_hbm, w2_ref.at[mine]), (h_hbm, h_ref), (x0_hbm, x0_ref)))]
    for copy in own:
        copy.start()
    barrier = pltpu.get_barrier_semaphore()

    @pl.loop(1, n_t)
    def _(q):
        pl.semaphore_signal(barrier, inc=1, device_id={'time': peer(q, 1)}, device_id_type=MESH_ID)
    for to in (up, down, far):
        pl.semaphore_signal(barrier, inc=1, device_id={'model': to}, device_id_type=MESH_ID)
    for copy in own:
        copy.wait()
    for j in range(span):
        hall[me_t, j:j + 1, :] = jnp.full((1, hall.shape[2]), h_ref[j], F32)
    pl.semaphore_wait(barrier, n_t + 2)

    for place in range(3):
        for i in range(2):
            mod_first(i, place).start()
    for d, to in lanes:
        for i in (d, 1 - d):
            w_first(i, d, to).start()

    @pl.loop(1, n_t)
    def _(q):
        h_time(q).start()

    for place in range(3):
        for i in range(2):
            mod_first(i, place).wait_recv()
    for i in range(2):
        modall[me_t, i] = jnp.concatenate([modraw[i, m].astype(F32) for m in range(n_m)], axis=1).astype(BF16)
    for qx in (1, 2, 3):
        mod_time(qx).start()
    mod_share(0).start()

    for d, to in lanes:
        w_first(d, d, to).wait_recv()
        w_forward(d, to).start()
        w_share(d, d).start()
    for d, to in lanes:
        w_first(1 - d, d, to).wait_recv()
        w_share(1 - d, d).start()
    for qx in (1, 2, 3):
        mod_time(qx).wait_recv()
        mod_share(qx).start()
    for d, to in lanes:
        w_forward(d, to).wait_recv()
        w_share(d, 2).start()

    @pl.loop(1, n_t)
    def _(q):
        h_time(q).wait_recv()
    for qx in range(n_x):
        mod_share(qx).wait_recv()

    @pl.loop(0, n_t)
    def _(t):
        sc_ref[t] = 0.5 * (1.0 + modall[t, 0].astype(F32))
        sh_ref[t] = 0.5 * modall[t, 1].astype(F32)

    for place in range(3):
        for i in range(2):
            w_share(i, place).wait_recv()
    for lo in range(0, hid, 128):
        w1_ref[:, lo:lo + 128] = w1t_ref[lo:lo + 128, :].T

    def drift(x, blocks, same):
        for lo, hi in chunks:
            p = jnp.dot(x, w1_ref[:, lo:hi], preferred_element_type=F32)
            for b, tb in enumerate(blocks):
                for j in range(span):
                    at = (b * span + j) * ROWS
                    v = (p if same else p[at:at + ROWS]) * sc_ref[tb, j:j + 1, lo:hi] + sh_ref[tb, j:j + 1, lo:hi]
                    t = jnp.tanh(v * (2 * ROOT + (8 * 0.044715 * ROOT) * (v * v)))
                    gbuf[at:at + ROWS, lo:hi] = (v + v * t).astype(BF16)
        return jnp.dot(gbuf[...], w2_ref[...], preferred_element_type=F32)

    def scaled(f, b, tb, j):
        at = (b * span + j) * ROWS
        h = hall[tb, j:j + 1, :]
        return f[at:at + ROWS] * jnp.concatenate([h] * (f.shape[1] // h.shape[1]), axis=1)

    def sweep(k, number):
        x0 = x0_ref[pl.ds(((k * n_m + me_m) * n_t + me_t) * ROWS, ROWS), :]

        def body(bx, acc):
            f = drift(x0.astype(BF16) if number == 0 else xbuf[k, bx], (2 * bx, 2 * bx + 1), number == 0)
            for b in range(2):
                if number == SWEEPS - 1:
                    obuf[k, 2 * bx + b] = acc
                for j in range(span):
                    if number < SWEEPS - 1:
                        at = (b * span + j) * ROWS
                        xbuf[k, bx, at:at + ROWS, :] = (x0 + acc).astype(BF16)
                    acc = acc + scaled(f, b, 2 * bx + b, j)
            return acc

        lax.fori_loop(0, n_x, body, jnp.zeros_like(x0))

    def sub(c):
        return pl.ds(c * block, block)

    def x_copy(k, q, to, src):
        return remote(xbuf.at[k, to // 2, sub(to % 2)], rbuf.at[0, k, src // 2, sub(src % 2)], s1s.at[k, q], s1r.at[k, q], time=to)

    def x_send(k):
        @pl.loop(1, n_t)
        def _(q):
            x_copy(k, q, peer(q, 1), me_t).start()
        rbuf[0, k, me_x, sub(me_c), :] = xbuf[k, me_x, sub(me_c), :]

    def x_ring(q, k, d, to):
        src = peer(q, -1)
        i = k * n_t + q
        return remote(rbuf.at[0, k, src // 2, sub(src % 2)], rbuf.at[1 + d, k, src // 2, sub(src % 2)], s2s.at[d, i], s2r.at[d, i], model=to)

    def x_next(q, k, d, to):
        src = peer(q, -1)
        i = k * n_t + q
        part = pl.ds((src % 2) * block + d * half, half)
        return remote(rbuf.at[1 + d, k, src // 2, part], rbuf.at[3, k, src // 2, part], s3s.at[d, i], s3r.at[d, i], model=to)

    def x_row(q, k):
        @pl.when(q > 0)
        def _():
            x_copy(k, q, me_t, peer(q, -1)).wait_recv()
        for d, to in lanes:
            x_ring(q, k, d, to).start()

    def x_pass(q, k):
        for d, to in lanes:
            x_ring(q, k, d, to).wait_recv()
            x_next(q, k, d, to).start()

    def x_far(q, k):
        for d, to in lanes:
            x_next(q, k, d, to).wait_recv()

    def o_copy(k, q, to, src):
        return remote(obuf.at[k, to], robuf.at[0, k, src], o1s.at[k, q], o1r.at[k, q], time=to)

    def o_ring(k, d, to):
        return remote(robuf.at[0, k], robuf.at[1 + d, k], o2s.at[d, k], o2r.at[d, k], model=to)

    def o_next(k, d, to):
        part = pl.ds(d * n_x, n_x)
        return remote(robuf.at[1 + d, k, part], robuf.at[3, k, part], o3s.at[d, k], o3r.at[d, k], model=to)

    def o_send(k):
        @pl.loop(1, n_t)
        def _(q):
            o_copy(k, q, peer(q, 1), me_t).start()
        robuf[0, k, me_t] = obuf[k, me_t]

    def o_row(k):
        @pl.loop(1, n_t)
        def _(q):
            o_copy(k, q, me_t, peer(q, -1)).wait_recv()
        for d, to in lanes:
            o_ring(k, d, to).start()

    def o_pass(k):
        for d, to in lanes:
            o_ring(k, d, to).wait_recv()
            o_next(k, d, to).start()

    def o_far(k):
        for d, to in lanes:
            o_next(k, d, to).wait_recv()

    def finish(rel, pair):
        k, src = pair // n_x, (me_x + n_x - hop(pair % n_x)) % n_x
        origin = (me_m + (n_m - rel) + (rel // 2) * (2 * rel - 5)) % n_m
        row = pl.multiple_of((((k * n_m + origin) * n_x + src) * 2) * ROWS, 2 * ROWS)
        f = drift(rbuf[rel, k, src], (me_t, me_t), False)
        for b in range(2):
            x0 = x0_ref[pl.ds(row + b * ROWS, ROWS), :]
            acc = robuf[rel, k, 2 * src + b]
            for j in range(span):
                out_ref[j, pl.ds(row + b * ROWS, ROWS), :] = x0 + acc
                acc = acc + scaled(f, b, me_t, j)

    @pl.loop(0, n_k * SWEEPS)
    def _(step):
        k, number = step // SWEEPS, step % SWEEPS

        @pl.when(number == 0)
        def _():
            sweep(k, 0)

        @pl.when(number % (SWEEPS - 1) > 0)
        def _():
            sweep(k, 1)

        @pl.when(number == SWEEPS - 2)
        def _():
            x_send(k)

        @pl.when(number == SWEEPS - 1)
        def _():
            sweep(k, SWEEPS - 1)
            o_send(k)

        @pl.when(step == SWEEPS - 2)
        def _():
            x_row(0, 0)

        @pl.when(step == SWEEPS - 1)
        def _():
            x_row(1, 0)

        @pl.when(step == SWEEPS)
        def _():
            x_pass(0, 0)
            x_row(2, 0)
            x_row(3, 0)

        @pl.when(step == SWEEPS + 1)
        def _():
            x_pass(1, 0)
            o_row(0)
            x_row(4, 0)
            x_row(5, 0)

        @pl.when(step == SWEEPS + 2)
        def _():
            x_pass(2, 0)
            x_pass(3, 0)
            o_pass(0)

    o_far(0)

    pairs = n_k * n_x
    early, ahead = 2, 3
    for c in range(2):
        x_row(ahead % n_x * 2 + c, ahead // n_x)

    @pl.loop(0, n_m * pairs)
    def _(n):
        p, turn = (n + 1) // n_m, (n + 1) % n_m
        rel, pair = (turn + n_m - 1) % n_m, p - (n_m - turn) // n_m

        @pl.when(turn == 0)
        def _():
            @pl.when(p < pairs)
            def _():
                @pl.when(p >= early)
                def _():
                    for c in range(2):
                        x_pass(p % n_x * 2 + c, p // n_x)

            @pl.when(p < pairs - ahead)
            def _():
                for c in range(2):
                    x_row((p + ahead) % n_x * 2 + c, (p + ahead) // n_x)

            @pl.when(p == 1)
            def _():
                o_row(1)

            @pl.when(p == 3)
            def _():
                o_pass(1)

            @pl.when(p == n_x)
            def _():
                o_far(1)

            for c in range(2):
                x_far(pair % n_x * 2 + c, pair // n_x)
        finish(rel, pair)

    for d, to in lanes:
        for i in range(2):
            w_first(i, d, to).wait_send()
        w_forward(d, to).wait_send()
    for place in range(3):
        for i in range(2):
            w_share(i, place).wait_send()
            mod_first(i, place).wait_send()
    for qx in range(n_x):
        if qx:
            mod_time(qx).wait_send()
        mod_share(qx).wait_send()

    @pl.loop(1, n_t)
    def _(q):
        h_time(q).wait_send()

    @pl.loop(0, n_k * n_t)
    def _(i):
        k, q = i // n_t, i % n_t

        @pl.when(q > 0)
        def _():
            x_copy(k, q, peer(q, 1), me_t).wait_send()
            o_copy(k, q, peer(q, 1), me_t).wait_send()
        for d, to in lanes:
            x_ring(q, k, d, to).wait_send()
            x_next(q, k, d, to).wait_send()
    for k in range(n_k):
        for d, to in lanes:
            o_ring(k, d, to).wait_send()
            o_next(k, d, to).wait_send()


def drain(n, src_ref, out_ref, sems):
    size = out_ref.shape[0] // n
    copies = [pltpu.make_async_copy(src_ref.at[pl.ds(i * size, size)], out_ref.at[pl.ds(i * size, size)], sems.at[i]) for i in range(n)]
    for copy in copies:
        copy.start()
    for copy in copies:
        copy.wait()


def solution(mesh):
    n_t, n_m = mesh.shape['time'], mesh.shape['model']

    def device_body(x_init, w_up, w_down, mod_scale, mod_shift, step_size):
        (span, hid_dev), chan = mod_scale.shape, x_init.shape[-1]
        rows = x_init.shape[0] * x_init.shape[1]
        hid = n_m * hid_dev
        n_k, n_x = rows // (n_t * n_m * ROWS), n_t // 2
        vmem = pl.BlockSpec(memory_space=pltpu.VMEM)
        sem = lambda *shape: pltpu.SemaphoreType.DMA(shape)
        hbm = pl.BlockSpec(memory_space=pltpu.HBM)
        out = pl.pallas_call(
            functools.partial(kernel, n_t, n_m),
            out_shape=pltpu.VMEM((span, rows, chan), F32),
            in_specs=[hbm] * 6,
            out_specs=vmem,
            scratch_shapes=[
                pltpu.SMEM((span,), F32),
                pltpu.VMEM((rows, chan), F32),
                pltpu.VMEM((chan, hid), BF16),
                pltpu.VMEM((hid, chan), BF16),
                pltpu.VMEM((hid, chan), BF16),
                pltpu.VMEM((2, n_m, span, hid_dev), BF16),
                pltpu.VMEM((n_t, 2, span, hid), BF16),
                pltpu.VMEM((n_t, span, 128), F32),
                pltpu.VMEM((n_t, span, hid), F32),
                pltpu.VMEM((n_t, span, hid), F32),
                pltpu.VMEM((n_k, n_x, 2 * span * ROWS, chan), BF16),
                pltpu.VMEM((n_k, n_t, ROWS, chan), F32),
                pltpu.VMEM((n_m, n_k, n_x, 2 * span * ROWS, chan), BF16),
                pltpu.VMEM((n_m, n_k, n_t, ROWS, chan), F32),
                pltpu.VMEM((2 * span * ROWS, hid), BF16),
                sem(6),
                sem(2, 2), sem(2, 2), sem(2), sem(2), sem(2, 3), sem(2, 3),
                sem(2, 3), sem(2, 3), sem(n_x), sem(n_x), sem(n_x), sem(n_x), sem(n_t), sem(n_t),
                sem(n_k, n_t), sem(n_k, n_t),
                sem(2, n_k * n_t), sem(2, n_k * n_t), sem(2, n_k * n_t), sem(2, n_k * n_t),
                sem(n_k, n_t), sem(n_k, n_t),
                sem(2, n_k), sem(2, n_k), sem(2, n_k), sem(2, n_k),
            ],
            compiler_params=pltpu.CompilerParams(collective_id=0, has_side_effects=True, vmem_limit_bytes=VMEM_BYTES - 4 * span * rows * chan),
        )(step_size, x_init.reshape(rows, chan), w_up.T, w_down, mod_scale, mod_shift)
        out = pl.pallas_call(
            functools.partial(drain, STAGES),
            out_shape=jax.ShapeDtypeStruct((span, rows, chan), F32),
            in_specs=[vmem],
            out_specs=hbm,
            scratch_shapes=[sem(STAGES)],
            compiler_params=pltpu.CompilerParams(vmem_limit_bytes=2 << 20),
        )(out)
        return out.reshape((span,) + x_init.shape)

    return jax.shard_map(device_body, mesh=mesh, in_specs=(P('data', None, None), P(None, 'model'), P('model', None), P('time', 'model'), P('time', 'model'), P('time')), out_specs=P('time', 'data', None, None), check_vma=False)
```

```python
import functools
import math

import jax
import jax.numpy as jnp
from jax import lax
from jax.experimental import pallas as pl
from jax.experimental.pallas import tpu as pltpu
from jax.sharding import PartitionSpec as P

SWEEPS = 4
VMEM_BYTES = 67043328
ROWS = 16
STAGES = 4
F32, BF16 = jnp.float32, jnp.bfloat16
MESH_ID = pl.DeviceIdType.MESH
ROOT = math.sqrt(2.0 / math.pi)


def kernel(n_t, n_m, h_hbm, x0_hbm, wu_hbm, wd_hbm, ms_hbm, mb_hbm, out_ref, h_ref, x0_ref, w1_ref, w1t_ref, w2_ref, modraw, modall, hall, sc_ref, sh_ref,
           xbuf, obuf, rbuf, robuf, gbuf, own_sem, gws, gwr, gfs, gfr, gds, gdr, ms, mr, mxs, mxr, mds, mdr, hs, hr,
           s1s, s1r, s2s, s2r, s3s, s3r, o1s, o1r, o2s, o2r, o3s, o3r):
    me_t = lax.axis_index('time')
    me_m = lax.axis_index('model')
    me_x, me_c = me_t // 2, me_t % 2
    n_g, n_x = obuf.shape[0], n_t // 2
    n_k = robuf.shape[1]
    block = xbuf.shape[2] // 2
    span = block // ROWS
    half = block // 2
    hid_dev = modraw.shape[3]
    hid = n_m * hid_dev
    chunks = ((0, 512), (512, hid))
    up, down, far = (me_m + 1) % n_m, (me_m + n_m - 1) % n_m, (me_m + 2) % n_m
    mate = me_x * 2 + (me_c + 1) % 2
    lanes = ((0, up), (1, down))

    def hop(qx):
        return qx + (qx // 2) * (5 - 2 * qx)

    def peer(q, sign):
        return ((me_x + n_x + sign * hop(q // 2)) % n_x) * 2 + (me_c + q % 2) % 2

    def remote(src, dst, send, recv, **where):
        return pltpu.make_async_remote_copy(src_ref=src, dst_ref=dst, send_sem=send, recv_sem=recv, device_id=where, device_id_type=MESH_ID)

    tables = (w1t_ref, w2_ref)

    def w_rows(origin, c):
        rows = hid_dev // 2
        return pl.ds(pl.multiple_of(origin * hid_dev + c * rows, 16), rows)

    def w_first(i, d, to):
        piece = tables[i].at[w_rows(me_m, me_c)]
        return remote(piece, piece, gws.at[i, d], gwr.at[i, d], model=to)

    def w_forward(d, to):
        piece = tables[d].at[w_rows((down, up)[d], me_c)]
        return remote(piece, piece, gfs.at[d], gfr.at[d], model=to)

    def w_share(i, place):
        piece = tables[i].at[w_rows((down, up, far)[place], me_c)]
        return remote(piece, piece, gds.at[i, place], gdr.at[i, place], time=mate)

    def mod_first(i, place):
        return remote(modraw.at[i, me_m], modraw.at[i, me_m], ms.at[i, place], mr.at[i, place], model=(up, down, far)[place])

    def mod_time(qx):
        return remote(modall.at[me_t], modall.at[me_t], mxs.at[qx], mxr.at[qx], time=((me_x + hop(qx)) % n_x) * 2 + me_c)

    def mod_share(qx):
        row = ((me_x + n_x - hop(qx)) % n_x) * 2 + me_c
        return remote(modall.at[row], modall.at[row], mds.at[qx], mdr.at[qx], time=mate)

    def h_time(q):
        return remote(hall.at[me_t], hall.at[me_t], hs.at[q], hr.at[q], time=peer(q, 1))

    def x0_of(g):
        origin = (me_m + 2 * (g // 2)) % n_m
        row = (((g + 1) // 2 * n_m + origin) * n_t + me_t) * ROWS
        return x0_ref[pl.ds(pl.multiple_of(row, ROWS), ROWS), :]

    mine = pl.ds(pl.multiple_of(me_m * hid_dev, 16), hid_dev)
    own = [pltpu.make_async_copy(src, dst, own_sem.at[i]) for i, (src, dst) in enumerate((
        (ms_hbm, modraw.at[0, me_m]), (mb_hbm, modraw.at[1, me_m]), (wu_hbm, w1t_ref.at[mine]), (wd_hbm, w2_ref.at[mine]), (h_hbm, h_ref), (x0_hbm, x0_ref)))]
    for copy in own:
        copy.start()
    barrier = pltpu.get_barrier_semaphore()

    @pl.loop(1, n_t)
    def _(q):
        pl.semaphore_signal(barrier, inc=1, device_id={'time': peer(q, 1)}, device_id_type=MESH_ID)
    for to in (up, down, far):
        pl.semaphore_signal(barrier, inc=1, device_id={'model': to}, device_id_type=MESH_ID)
    for copy in own:
        copy.wait()
    for j in range(span):
        hall[me_t, j:j + 1, :] = jnp.full((1, hall.shape[2]), h_ref[j], F32)
    pl.semaphore_wait(barrier, n_t + 2)

    for place in range(3):
        for i in range(2):
            mod_first(i, place).start()
    for d, to in lanes:
        for i in (d, 1 - d):
            w_first(i, d, to).start()

    @pl.loop(1, n_t)
    def _(q):
        h_time(q).start()

    @pl.loop(0, n_g * n_x)
    def _(i):
        xbuf[i // n_x, i % n_x] = jnp.concatenate([x0_of(i // n_x).astype(BF16)] * (2 * span), axis=0)

    for place in range(3):
        for i in range(2):
            mod_first(i, place).wait_recv()
    for i in range(2):
        modall[me_t, i] = jnp.concatenate([modraw[i, m].astype(F32) for m in range(n_m)], axis=1).astype(BF16)
    for qx in (1, 2, 3):
        mod_time(qx).start()
    mod_share(0).start()

    for d, to in lanes:
        w_first(d, d, to).wait_recv()
        w_forward(d, to).start()
        w_share(d, d).start()
    for d, to in lanes:
        w_first(1 - d, d, to).wait_recv()
        w_share(1 - d, d).start()
    for qx in (1, 2, 3):
        mod_time(qx).wait_recv()
        mod_share(qx).start()
    for d, to in lanes:
        w_forward(d, to).wait_recv()
        w_share(d, 2).start()

    @pl.loop(1, n_t)
    def _(q):
        h_time(q).wait_recv()
    for qx in range(n_x):
        mod_share(qx).wait_recv()

    @pl.loop(0, n_t)
    def _(t):
        sc_ref[t] = 0.5 * (1.0 + modall[t, 0].astype(F32))
        sh_ref[t] = 0.5 * modall[t, 1].astype(F32)

    for place in range(3):
        for i in range(2):
            w_share(i, place).wait_recv()
    for lo in range(0, hid, 128):
        w1_ref[:, lo:lo + 128] = w1t_ref[lo:lo + 128, :].T

    def lift(slot, x, blocks):
        for lo, hi in chunks:
            p = jnp.dot(x, w1_ref[:, lo:hi], preferred_element_type=F32)
            for b, tb in enumerate(blocks):
                for j in range(span):
                    at = (b * span + j) * ROWS
                    v = p[at:at + ROWS] * sc_ref[tb, j:j + 1, lo:hi] + sh_ref[tb, j:j + 1, lo:hi]
                    t = jnp.tanh(v * (2 * ROOT + (8 * 0.044715 * ROOT) * (v * v)))
                    gbuf[slot, at:at + ROWS, lo:hi] = (v + v * t).astype(BF16)

    def lower(slot):
        return jnp.dot(gbuf[slot], w2_ref[...], preferred_element_type=F32)

    def scaled(f, b, tb, j):
        at = (b * span + j) * ROWS
        h = hall[tb, j:j + 1, :]
        return f[at:at + ROWS] * jnp.concatenate([h] * (f.shape[1] // h.shape[1]), axis=1)

    def place_of(g):
        return 3 * (g // 2), (g + 1) // 2

    def sweep(g, number):
        x0 = x0_of(g)
        to = g + number // (SWEEPS - 1) * (n_g - g)
        acc = jnp.zeros_like(x0)
        lift(0, xbuf[g, 0], (0, 1))
        for bx in range(n_x):
            if bx + 1 < n_x:
                lift((bx + 1) % 2, xbuf[g, bx + 1], (2 * bx + 2, 2 * bx + 3))
            f = lower(bx % 2)
            for b in range(2):
                obuf[g, 2 * bx + b] = acc
                for j in range(span):
                    at = (b * span + j) * ROWS
                    xbuf[to, bx, at:at + ROWS, :] = (x0 + acc).astype(BF16)
                    acc = acc + scaled(f, b, 2 * bx + b, j)

    def sub(c):
        return pl.ds(c * block, block)

    def x_copy(g, q, to, src):
        rel, k = place_of(g)
        return remote(xbuf.at[g, to // 2, sub(to % 2)], rbuf.at[rel, k, src // 2, sub(src % 2)], s1s.at[g, q], s1r.at[g, q], time=to)

    def x_send(g):
        @pl.loop(1, n_t)
        def _(q):
            x_copy(g, q, peer(q, 1), me_t).start()
        rel, k = place_of(g)
        rbuf[rel, k, me_x, sub(me_c), :] = xbuf[g, me_x, sub(me_c), :]

    def x_come(g, q):
        @pl.when(q > 0)
        def _():
            x_copy(g, q, me_t, peer(q, -1)).wait_recv()

    def x_ring(q, k, d, to):
        src = peer(q, -1)
        i = k * n_t + q
        return remote(rbuf.at[0, k, src // 2, sub(src % 2)], rbuf.at[1 + d, k, src // 2, sub(src % 2)], s2s.at[d, i], s2r.at[d, i], model=to)

    def x_next(q, k, d, to):
        src = peer(q, -1)
        i = k * n_t + q
        part = pl.ds((src % 2) * block + d * half, half)
        return remote(rbuf.at[1 + d, k, src // 2, part], rbuf.at[3, k, src // 2, part], s3s.at[d, i], s3r.at[d, i], model=to)

    def x_row(q, k):
        x_come(k, q)
        for d, to in lanes:
            x_ring(q, k, d, to).start()

    def x_pass(q, k):
        for d, to in lanes:
            x_ring(q, k, d, to).wait_recv()
            x_next(q, k, d, to).start()

    def x_far(q, k):
        for d, to in lanes:
            x_next(q, k, d, to).wait_recv()

    def o_copy(g, q, to, src):
        rel, k = place_of(g)
        return remote(obuf.at[g, to], robuf.at[rel, k, src], o1s.at[g, q], o1r.at[g, q], time=to)

    def o_ring(k, d, to):
        return remote(robuf.at[0, k], robuf.at[1 + d, k], o2s.at[d, k], o2r.at[d, k], model=to)

    def o_next(k, d, to):
        part = pl.ds(d * n_x, n_x)
        return remote(robuf.at[1 + d, k, part], robuf.at[3, k, part], o3s.at[d, k], o3r.at[d, k], model=to)

    def o_send(g):
        @pl.loop(1, n_t)
        def _(q):
            o_copy(g, q, peer(q, 1), me_t).start()
        rel, k = place_of(g)
        robuf[rel, k, me_t] = obuf[g, me_t]

    def o_come(g):
        @pl.loop(1, n_t)
        def _(q):
            o_copy(g, q, me_t, peer(q, -1)).wait_recv()

    def o_row(k):
        o_come(k)
        for d, to in lanes:
            o_ring(k, d, to).start()

    def o_pass(k):
        for d, to in lanes:
            o_ring(k, d, to).wait_recv()
            o_next(k, d, to).start()

    def o_far(k):
        for d, to in lanes:
            o_next(k, d, to).wait_recv()

    def finish(rels, pair):
        k, src = pair // n_x, (me_x + n_x - hop(pair % n_x)) % n_x
        for slot, rel in enumerate(rels):
            lift(slot, rbuf[rel, k, src], (me_t, me_t))
        for slot, rel in enumerate(rels):
            origin = (me_m + (n_m - rel) + (rel // 2) * (2 * rel - 5)) % n_m
            row = pl.multiple_of((((k * n_m + origin) * n_x + src) * 2) * ROWS, 2 * ROWS)
            f = lower(slot)
            for b in range(2):
                x0 = x0_ref[pl.ds(row + b * ROWS, ROWS), :]
                acc = robuf[rel, k, 2 * src + b]
                for j in range(span):
                    out_ref[j, pl.ds(row + b * ROWS, ROWS), :] = x0 + acc
                    acc = acc + scaled(f, b, me_t, j)

    def row_at(i):
        x_row(i % n_t, i // n_t)

    @pl.loop(0, n_g * SWEEPS)
    def _(step):
        g, number = step // SWEEPS, step % SWEEPS
        sweep(g, number)

        @pl.when(number == SWEEPS - 2)
        def _():
            x_send(g)

        @pl.when(number == SWEEPS - 1)
        def _():
            o_send(g)

        @pl.when(step == 2)
        def _():
            row_at(0)

        @pl.when(step == 3)
        def _():
            row_at(1)

        @pl.when(step == 4)
        def _():
            row_at(2)

        @pl.when(step > 3)
        def _():
            row_at(step - 1)

        @pl.when(step > 4)
        def _():
            x_pass(step - 5, 0)

        @pl.when(step == 5)
        def _():
            o_row(0)

        @pl.when(step == 7)
        def _():
            o_pass(0)

        @pl.when(step == 9)
        def _():
            o_row(1)

    passed = n_g * SWEEPS - 5
    rowed = n_g * SWEEPS - 1
    for q in range(passed, n_t):
        x_pass(q, 0)
    o_far(0)

    @pl.loop(0, n_k * n_x * 2)
    def _(i):
        pair, part = i // 2, i % 2
        k, at = pair // n_x, pair % n_x * 2

        @pl.when(part == 0)
        def _():
            @pl.when(pair + rowed < n_k * n_t)
            def _():
                row_at(pair + rowed)

            @pl.when(pair == n_x)
            def _():
                for d, to in lanes:
                    o_ring(1, d, to).wait_recv()
                o_come(2)

            @pl.when(k == 1)
            def _():
                for c in range(2):
                    x_ring(at + c, 1, 0, up).wait_recv()

        @pl.when(part == 1)
        def _():
            @pl.when(k == 0)
            def _():
                for c in range(2):
                    x_far(at + c, 0)

            @pl.when(k == 1)
            def _():
                for c in range(2):
                    x_ring(at + c, 1, 1, down).wait_recv()
                    x_come(2, at + c)
        finish((2 * part, 2 * part + 1), pair)

    for d, to in lanes:
        for i in range(2):
            w_first(i, d, to).wait_send()
        w_forward(d, to).wait_send()
    for place in range(3):
        for i in range(2):
            w_share(i, place).wait_send()
            mod_first(i, place).wait_send()
    for qx in range(n_x):
        if qx:
            mod_time(qx).wait_send()
        mod_share(qx).wait_send()

    @pl.loop(1, n_t)
    def _(q):
        h_time(q).wait_send()

    @pl.loop(0, n_g * n_t)
    def _(i):
        g, q = i // n_t, i % n_t

        @pl.when(q > 0)
        def _():
            x_copy(g, q, peer(q, 1), me_t).wait_send()
            o_copy(g, q, peer(q, 1), me_t).wait_send()

    @pl.loop(0, n_k * n_t)
    def _(i):
        for d, to in lanes:
            x_ring(i % n_t, i // n_t, d, to).wait_send()

    @pl.loop(0, n_t)
    def _(q):
        for d, to in lanes:
            x_next(q, 0, d, to).wait_send()
    for d, to in lanes:
        for k in range(n_k):
            o_ring(k, d, to).wait_send()
        o_next(0, d, to).wait_send()


def drain(n, src_ref, out_ref, sems):
    size = out_ref.shape[0] // n
    copies = [pltpu.make_async_copy(src_ref.at[pl.ds(i * size, size)], out_ref.at[pl.ds(i * size, size)], sems.at[i]) for i in range(n)]
    for copy in copies:
        copy.start()
    for copy in copies:
        copy.wait()


def solution(mesh):
    n_t, n_m = mesh.shape['time'], mesh.shape['model']

    def device_body(x_init, w_up, w_down, mod_scale, mod_shift, step_size):
        (span, hid_dev), chan = mod_scale.shape, x_init.shape[-1]
        rows = x_init.shape[0] * x_init.shape[1]
        hid = n_m * hid_dev
        n_k, n_x = rows // (n_t * n_m * ROWS), n_t // 2
        n_g = n_k + 1
        vmem = pl.BlockSpec(memory_space=pltpu.VMEM)
        sem = lambda *shape: pltpu.SemaphoreType.DMA(shape)
        hbm = pl.BlockSpec(memory_space=pltpu.HBM)
        out = pl.pallas_call(
            functools.partial(kernel, n_t, n_m),
            out_shape=pltpu.VMEM((span, rows, chan), F32),
            in_specs=[hbm] * 6,
            out_specs=vmem,
            scratch_shapes=[
                pltpu.SMEM((span,), F32),
                pltpu.VMEM((rows, chan), F32),
                pltpu.VMEM((chan, hid), BF16),
                pltpu.VMEM((hid, chan), BF16),
                pltpu.VMEM((hid, chan), BF16),
                pltpu.VMEM((2, n_m, span, hid_dev), BF16),
                pltpu.VMEM((n_t, 2, span, hid), BF16),
                pltpu.VMEM((n_t, span, 128), F32),
                pltpu.VMEM((n_t, span, hid), F32),
                pltpu.VMEM((n_t, span, hid), F32),
                pltpu.VMEM((n_g + 1, n_x, 2 * span * ROWS, chan), BF16),
                pltpu.VMEM((n_g, n_t, ROWS, chan), F32),
                pltpu.VMEM((n_m, n_k, n_x, 2 * span * ROWS, chan), BF16),
                pltpu.VMEM((n_m, n_k, n_t, ROWS, chan), F32),
                pltpu.VMEM((2, 2 * span * ROWS, hid), BF16),
                sem(6),
                sem(2, 2), sem(2, 2), sem(2), sem(2), sem(2, 3), sem(2, 3),
                sem(2, 3), sem(2, 3), sem(n_x), sem(n_x), sem(n_x), sem(n_x), sem(n_t), sem(n_t),
                sem(n_g, n_t), sem(n_g, n_t),
                sem(2, n_k * n_t), sem(2, n_k * n_t), sem(2, n_t), sem(2, n_t),
                sem(n_g, n_t), sem(n_g, n_t),
                sem(2, n_k), sem(2, n_k), sem(2, n_k), sem(2, n_k),
            ],
            compiler_params=pltpu.CompilerParams(collective_id=0, has_side_effects=True, vmem_limit_bytes=VMEM_BYTES - 4 * span * rows * chan),
        )(step_size, x_init.reshape(rows, chan), w_up.T, w_down, mod_scale, mod_shift)
        out = pl.pallas_call(
            functools.partial(drain, STAGES),
            out_shape=jax.ShapeDtypeStruct((span, rows, chan), F32),
            in_specs=[vmem],
            out_specs=hbm,
            scratch_shapes=[sem(STAGES)],
            compiler_params=pltpu.CompilerParams(vmem_limit_bytes=2 << 20),
        )(out)
        return out.reshape((span,) + x_init.shape)

    return jax.shard_map(device_body, mesh=mesh, in_specs=(P('data', None, None), P(None, 'model'), P('model', None), P('time', 'model'), P('time', 'model'), P('time')), out_specs=P('time', 'data', None, None), check_vma=False)
```

```python
import functools
import math

import jax
import jax.numpy as jnp
from jax import lax
from jax.experimental import pallas as pl
from jax.experimental.pallas import tpu as pltpu
from jax.sharding import PartitionSpec as P

SWEEPS = 4
VMEM_BYTES = 67043328
ROWS = 16
STAGES = 4
F32, BF16 = jnp.float32, jnp.bfloat16
MESH_ID = pl.DeviceIdType.MESH
ROOT = math.sqrt(2.0 / math.pi)


def kernel(n_t, n_m, h_hbm, x0_hbm, wu_hbm, wd_hbm, ms_hbm, mb_hbm, out_ref, h_ref, x0_ref, w1_ref, w1t_ref, w2_ref, modraw, modall, hall, sc_ref, sh_ref,
           xbuf, obuf, rbuf, robuf, gbuf, own_sem, gws, gwr, gfs, gfr, gds, gdr, ms, mr, mxs, mxr, mds, mdr, hs, hr,
           s1s, s1r, s2s, s2r, s3s, s3r, o1s, o1r, o2s, o2r, o3s, o3r):
    me_t = lax.axis_index('time')
    me_m = lax.axis_index('model')
    me_x, me_c = me_t // 2, me_t % 2
    n_g, n_x = obuf.shape[0], n_t // 2
    n_k = robuf.shape[1]
    block = xbuf.shape[2] // 2
    span = block // ROWS
    half = block // 2
    hid_dev = modraw.shape[3]
    hid = n_m * hid_dev
    chunks = [(lo, min(lo + 256, hid)) for lo in range(0, hid, 256)]
    up, down, far = (me_m + 1) % n_m, (me_m + n_m - 1) % n_m, (me_m + 2) % n_m
    mate = me_x * 2 + (me_c + 1) % 2
    lanes = ((0, up), (1, down))

    def hop(qx):
        return qx + (qx // 2) * (5 - 2 * qx)

    def peer(q, sign):
        return ((me_x + n_x + sign * hop(q // 2)) % n_x) * 2 + (me_c + q % 2) % 2

    def remote(src, dst, send, recv, **where):
        return pltpu.make_async_remote_copy(src_ref=src, dst_ref=dst, send_sem=send, recv_sem=recv, device_id=where, device_id_type=MESH_ID)

    tables = (w1t_ref, w2_ref)

    def w_rows(origin, c):
        rows = hid_dev // 2
        return pl.ds(pl.multiple_of(origin * hid_dev + c * rows, 16), rows)

    def w_first(i, d, to):
        piece = tables[i].at[w_rows(me_m, me_c)]
        return remote(piece, piece, gws.at[i, d], gwr.at[i, d], model=to)

    def w_forward(d, to):
        piece = tables[d].at[w_rows((down, up)[d], me_c)]
        return remote(piece, piece, gfs.at[d], gfr.at[d], model=to)

    def w_share(i, place):
        piece = tables[i].at[w_rows((down, up, far)[place], me_c)]
        return remote(piece, piece, gds.at[i, place], gdr.at[i, place], time=mate)

    def mod_first(i, place):
        return remote(modraw.at[i, me_m], modraw.at[i, me_m], ms.at[i, place], mr.at[i, place], model=(up, down, far)[place])

    def mod_time(qx):
        return remote(modall.at[me_t], modall.at[me_t], mxs.at[qx], mxr.at[qx], time=((me_x + hop(qx)) % n_x) * 2 + me_c)

    def mod_share(qx):
        row = ((me_x + n_x - hop(qx)) % n_x) * 2 + me_c
        return remote(modall.at[row], modall.at[row], mds.at[qx], mdr.at[qx], time=mate)

    def h_time(q):
        return remote(hall.at[me_t], hall.at[me_t], hs.at[q], hr.at[q], time=peer(q, 1))

    def x0_of(g):
        origin = (me_m + 2 * (g // 2)) % n_m
        row = (((g + 1) // 2 * n_m + origin) * n_t + me_t) * ROWS
        return x0_ref[pl.ds(pl.multiple_of(row, ROWS), ROWS), :]

    mine = pl.ds(pl.multiple_of(me_m * hid_dev, 16), hid_dev)
    own = [pltpu.make_async_copy(src, dst, own_sem.at[i]) for i, (src, dst) in enumerate((
        (ms_hbm, modraw.at[0, me_m]), (mb_hbm, modraw.at[1, me_m]), (wu_hbm, w1t_ref.at[mine]), (wd_hbm, w2_ref.at[mine]), (h_hbm, h_ref), (x0_hbm, x0_ref)))]
    for copy in own:
        copy.start()
    barrier = pltpu.get_barrier_semaphore()

    @pl.loop(1, n_t)
    def _(q):
        pl.semaphore_signal(barrier, inc=1, device_id={'time': peer(q, 1)}, device_id_type=MESH_ID)
    for to in (up, down, far):
        pl.semaphore_signal(barrier, inc=1, device_id={'model': to}, device_id_type=MESH_ID)
    for copy in own:
        copy.wait()
    for j in range(span):
        hall[me_t, j:j + 1, :] = jnp.full((1, hall.shape[2]), h_ref[j], F32)
    pl.semaphore_wait(barrier, n_t + 2)

    for place in range(3):
        for i in range(2):
            mod_first(i, place).start()
    for d, to in lanes:
        for i in (d, 1 - d):
            w_first(i, d, to).start()

    @pl.loop(1, n_t)
    def _(q):
        h_time(q).start()

    @pl.loop(0, n_g * n_x)
    def _(i):
        xbuf[i // n_x, i % n_x] = jnp.concatenate([x0_of(i // n_x).astype(BF16)] * (2 * span), axis=0)

    for place in range(3):
        for i in range(2):
            mod_first(i, place).wait_recv()
    for i in range(2):
        modall[me_t, i] = jnp.concatenate([modraw[i, m].astype(F32) for m in range(n_m)], axis=1).astype(BF16)
    for qx in (1, 2, 3):
        mod_time(qx).start()
    mod_share(0).start()

    for d, to in lanes:
        w_first(d, d, to).wait_recv()
        w_forward(d, to).start()
        w_share(d, d).start()
    for d, to in lanes:
        w_first(1 - d, d, to).wait_recv()
        w_share(1 - d, d).start()
    for qx in (1, 2, 3):
        mod_time(qx).wait_recv()
        mod_share(qx).start()
    for d, to in lanes:
        w_forward(d, to).wait_recv()
        w_share(d, 2).start()

    @pl.loop(1, n_t)
    def _(q):
        h_time(q).wait_recv()
    for qx in range(n_x):
        mod_share(qx).wait_recv()

    @pl.loop(0, n_t)
    def _(t):
        sc_ref[t] = 0.5 * (1.0 + modall[t, 0].astype(F32))
        sh_ref[t] = 0.5 * modall[t, 1].astype(F32)

    for place in range(3):
        for i in range(2):
            w_share(i, place).wait_recv()
    for lo in range(0, hid, 128):
        w1_ref[:, lo:lo + 128] = w1t_ref[lo:lo + 128, :].T

    def lift(slot, x, blocks):
        for lo, hi in chunks:
            p = jnp.dot(x, w1_ref[:, lo:hi], preferred_element_type=F32)
            for b, tb in enumerate(blocks):
                for j in range(span):
                    at = (b * span + j) * ROWS
                    v = p[at:at + ROWS] * sc_ref[tb, j:j + 1, lo:hi] + sh_ref[tb, j:j + 1, lo:hi]
                    t = jnp.tanh(v * (2 * ROOT + (8 * 0.044715 * ROOT) * (v * v)))
                    gbuf[slot, at:at + ROWS, lo:hi] = (v + v * t).astype(BF16)

    def lower(slot):
        return jnp.dot(gbuf[slot], w2_ref[...], preferred_element_type=F32)

    def scaled(f, b, tb, j):
        at = (b * span + j) * ROWS
        h = hall[tb, j:j + 1, :]
        return f[at:at + ROWS] * jnp.concatenate([h] * (f.shape[1] // h.shape[1]), axis=1)

    def place_of(g):
        return 3 * (g // 2), (g + 1) // 2

    def sweep(g, number):
        x0 = x0_of(g)
        to = g + number // (SWEEPS - 1) * (n_g - g)
        acc = jnp.zeros_like(x0)
        lift(0, xbuf[g, 0], (0, 1))
        for bx in range(n_x):
            if bx + 1 < n_x:
                lift((bx + 1) % 2, xbuf[g, bx + 1], (2 * bx + 2, 2 * bx + 3))
            f = lower(bx % 2)
            for b in range(2):
                obuf[g, 2 * bx + b] = acc
                for j in range(span):
                    at = (b * span + j) * ROWS
                    xbuf[to, bx, at:at + ROWS, :] = (x0 + acc).astype(BF16)
                    acc = acc + scaled(f, b, 2 * bx + b, j)

    def sub(c):
        return pl.ds(c * block, block)

    def x_copy(g, q, to, src):
        rel, k = place_of(g)
        return remote(xbuf.at[g, to // 2, sub(to % 2)], rbuf.at[rel, k, src // 2, sub(src % 2)], s1s.at[g, q], s1r.at[g, q], time=to)

    def x_send(g):
        @pl.loop(1, n_t)
        def _(q):
            x_copy(g, q, peer(q, 1), me_t).start()
        rel, k = place_of(g)
        rbuf[rel, k, me_x, sub(me_c), :] = xbuf[g, me_x, sub(me_c), :]

    def x_come(g, q):
        @pl.when(q > 0)
        def _():
            x_copy(g, q, me_t, peer(q, -1)).wait_recv()

    def x_ring(q, k, d, to):
        src = peer(q, -1)
        i = k * n_t + q
        return remote(rbuf.at[0, k, src // 2, sub(src % 2)], rbuf.at[1 + d, k, src // 2, sub(src % 2)], s2s.at[d, i], s2r.at[d, i], model=to)

    def x_next(q, k, d, to):
        src = peer(q, -1)
        i = k * n_t + q
        part = pl.ds((src % 2) * block + d * half, half)
        return remote(rbuf.at[1 + d, k, src // 2, part], rbuf.at[3, k, src // 2, part], s3s.at[d, i], s3r.at[d, i], model=to)

    def x_row(q, k):
        x_come(k, q)
        for d, to in lanes:
            x_ring(q, k, d, to).start()

    def x_pass(q, k):
        for d, to in lanes:
            x_ring(q, k, d, to).wait_recv()
            x_next(q, k, d, to).start()

    def x_far(q, k):
        for d, to in lanes:
            x_next(q, k, d, to).wait_recv()

    def o_copy(g, q, to, src):
        rel, k = place_of(g)
        return remote(obuf.at[g, to], robuf.at[rel, k, src], o1s.at[g, q], o1r.at[g, q], time=to)

    def o_ring(k, d, to):
        return remote(robuf.at[0, k], robuf.at[1 + d, k], o2s.at[d, k], o2r.at[d, k], model=to)

    def o_next(k, d, to):
        part = pl.ds(d * n_x, n_x)
        return remote(robuf.at[1 + d, k, part], robuf.at[3, k, part], o3s.at[d, k], o3r.at[d, k], model=to)

    def o_send(g):
        @pl.loop(1, n_t)
        def _(q):
            o_copy(g, q, peer(q, 1), me_t).start()
        rel, k = place_of(g)
        robuf[rel, k, me_t] = obuf[g, me_t]

    def o_come(g):
        @pl.loop(1, n_t)
        def _(q):
            o_copy(g, q, me_t, peer(q, -1)).wait_recv()

    def o_row(k):
        o_come(k)
        for d, to in lanes:
            o_ring(k, d, to).start()

    def o_pass(k):
        for d, to in lanes:
            o_ring(k, d, to).wait_recv()
            o_next(k, d, to).start()

    def o_far(k):
        for d, to in lanes:
            o_next(k, d, to).wait_recv()

    def finish(rels, pair):
        k, src = pair // n_x, (me_x + n_x - hop(pair % n_x)) % n_x
        for slot, rel in enumerate(rels):
            lift(slot, rbuf[rel, k, src], (me_t, me_t))
            origin = (me_m + (n_m - rel) + (rel // 2) * (2 * rel - 5)) % n_m
            row = pl.multiple_of((((k * n_m + origin) * n_x + src) * 2) * ROWS, 2 * ROWS)
            f = lower(slot)
            for b in range(2):
                x0 = x0_ref[pl.ds(row + b * ROWS, ROWS), :]
                acc = robuf[rel, k, 2 * src + b]
                for j in range(span):
                    out_ref[j, pl.ds(row + b * ROWS, ROWS), :] = x0 + acc
                    acc = acc + scaled(f, b, me_t, j)

    def row_at(i):
        x_row(i % n_t, i // n_t)

    @pl.loop(0, n_g * SWEEPS - 1)
    def _(step):
        g, number = step // SWEEPS, step % SWEEPS
        sweep(g, number)

        @pl.when(number == SWEEPS - 2)
        def _():
            x_send(g)

        @pl.when(number == SWEEPS - 1)
        def _():
            o_send(g)

        @pl.when(step == 2)
        def _():
            row_at(0)

        @pl.when(step == 3)
        def _():
            row_at(1)

        @pl.when(step == 4)
        def _():
            row_at(2)

        @pl.when(step > 3)
        def _():
            row_at(step - 1)

        @pl.when(step > 4)
        def _():
            x_pass(step - 5, 0)

        @pl.when(step == 5)
        def _():
            o_row(0)

        @pl.when(step == 7)
        def _():
            o_pass(0)

        @pl.when(step == 9)
        def _():
            o_row(1)

    passed, rowed = n_g * SWEEPS - 6, n_g * SWEEPS - 2
    o_far(0)
    for q in range(passed, n_t - 1):
        x_pass(q, 0)

    @pl.loop(0, n_k * n_x * 2)
    def _(i):
        pair, part = i // 2, i % 2
        k, at = pair // n_x, pair % n_x * 2

        @pl.when(part == 0)
        def _():
            @pl.when(pair + rowed < n_k * n_t)
            def _():
                row_at(pair + rowed)

            @pl.when(pair == 1)
            def _():
                o_pass(1)

            @pl.when(pair == n_x)
            def _():
                o_far(1)

            @pl.when(k == 1)
            def _():
                for c in range(2):
                    x_ring(at + c, 1, 0, up).wait_recv()

        @pl.when(part == 1)
        def _():
            @pl.when(pair == 0)
            def _():
                x_pass(n_t - 1, 0)

            @pl.when(k == 0)
            def _():
                for c in range(2):
                    x_far(at + c, 0)

            @pl.when(k == 1)
            def _():
                for c in range(2):
                    x_ring(at + c, 1, 1, down).wait_recv()
                    x_come(2, at + c)
        finish((2 * part, 2 * part + 1), pair)

    for d, to in lanes:
        for i in range(2):
            w_first(i, d, to).wait_send()
        w_forward(d, to).wait_send()
    for place in range(3):
        for i in range(2):
            w_share(i, place).wait_send()
            mod_first(i, place).wait_send()
    for qx in range(n_x):
        if qx:
            mod_time(qx).wait_send()
        mod_share(qx).wait_send()

    @pl.loop(1, n_t)
    def _(q):
        h_time(q).wait_send()

    @pl.loop(0, n_g * n_t)
    def _(i):
        g, q = i // n_t, i % n_t

        @pl.when(q > 0)
        def _():
            x_copy(g, q, peer(q, 1), me_t).wait_send()

            @pl.when(g < n_k)
            def _():
                o_copy(g, q, peer(q, 1), me_t).wait_send()

    @pl.loop(0, n_k * n_t)
    def _(i):
        for d, to in lanes:
            x_ring(i % n_t, i // n_t, d, to).wait_send()

    @pl.loop(0, n_t)
    def _(q):
        for d, to in lanes:
            x_next(q, 0, d, to).wait_send()
    for d, to in lanes:
        for k in range(n_k):
            o_ring(k, d, to).wait_send()
            o_next(k, d, to).wait_send()


def drain(n, src_ref, out_ref, sems):
    size = out_ref.shape[0] // n
    copies = [pltpu.make_async_copy(src_ref.at[pl.ds(i * size, size)], out_ref.at[pl.ds(i * size, size)], sems.at[i]) for i in range(n)]
    for copy in copies:
        copy.start()
    for copy in copies:
        copy.wait()


def solution(mesh):
    n_t, n_m = mesh.shape['time'], mesh.shape['model']

    def device_body(x_init, w_up, w_down, mod_scale, mod_shift, step_size):
        (span, hid_dev), chan = mod_scale.shape, x_init.shape[-1]
        rows = x_init.shape[0] * x_init.shape[1]
        hid = n_m * hid_dev
        n_k, n_x = rows // (n_t * n_m * ROWS), n_t // 2
        n_g = n_k + 1
        vmem = pl.BlockSpec(memory_space=pltpu.VMEM)
        sem = lambda *shape: pltpu.SemaphoreType.DMA(shape)
        hbm = pl.BlockSpec(memory_space=pltpu.HBM)
        out = pl.pallas_call(
            functools.partial(kernel, n_t, n_m),
            out_shape=pltpu.VMEM((span, rows, chan), F32),
            in_specs=[hbm] * 6,
            out_specs=vmem,
            scratch_shapes=[
                pltpu.SMEM((span,), F32),
                pltpu.VMEM((rows, chan), F32),
                pltpu.VMEM((chan, hid), BF16),
                pltpu.VMEM((hid, chan), BF16),
                pltpu.VMEM((hid, chan), BF16),
                pltpu.VMEM((2, n_m, span, hid_dev), BF16),
                pltpu.VMEM((n_t, 2, span, hid), BF16),
                pltpu.VMEM((n_t, span, 128), F32),
                pltpu.VMEM((n_t, span, hid), F32),
                pltpu.VMEM((n_t, span, hid), F32),
                pltpu.VMEM((n_g + 1, n_x, 2 * span * ROWS, chan), BF16),
                pltpu.VMEM((n_g, n_t, ROWS, chan), F32),
                pltpu.VMEM((n_m, n_k, n_x, 2 * span * ROWS, chan), BF16),
                pltpu.VMEM((n_m, n_k, n_t, ROWS, chan), F32),
                pltpu.VMEM((2, 2 * span * ROWS, hid), BF16),
                sem(6),
                sem(2, 2), sem(2, 2), sem(2), sem(2), sem(2, 3), sem(2, 3),
                sem(2, 3), sem(2, 3), sem(n_x), sem(n_x), sem(n_x), sem(n_x), sem(n_t), sem(n_t),
                sem(n_g, n_t), sem(n_g, n_t),
                sem(2, n_k * n_t), sem(2, n_k * n_t), sem(2, n_t), sem(2, n_t),
                sem(n_g, n_t), sem(n_g, n_t),
                sem(2, n_k), sem(2, n_k), sem(2, n_k), sem(2, n_k),
            ],
            compiler_params=pltpu.CompilerParams(collective_id=0, has_side_effects=True, vmem_limit_bytes=VMEM_BYTES - 4 * span * rows * chan),
        )(step_size, x_init.reshape(rows, chan), w_up.T, w_down, mod_scale, mod_shift)
        out = pl.pallas_call(
            functools.partial(drain, STAGES),
            out_shape=jax.ShapeDtypeStruct((span, rows, chan), F32),
            in_specs=[vmem],
            out_specs=hbm,
            scratch_shapes=[sem(STAGES)],
            compiler_params=pltpu.CompilerParams(vmem_limit_bytes=2 << 20),
        )(out)
        return out.reshape((span,) + x_init.shape)

    return jax.shard_map(device_body, mesh=mesh, in_specs=(P('data', None, None), P(None, 'model'), P('model', None), P('time', 'model'), P('time', 'model'), P('time')), out_specs=P('time', 'data', None, None), check_vma=False)
```

```python
import functools
import math

import jax
import jax.numpy as jnp
from jax import lax
from jax.experimental import pallas as pl
from jax.experimental.pallas import tpu as pltpu
from jax.sharding import PartitionSpec as P

SWEEPS = 4
VMEM_BYTES = 67043328
ROWS = 16
STAGES = 4
F32, BF16 = jnp.float32, jnp.bfloat16
MESH_ID = pl.DeviceIdType.MESH
ROOT = math.sqrt(2.0 / math.pi)


def kernel(n_t, n_m, h_hbm, x0_hbm, wu_hbm, wd_hbm, ms_hbm, mb_hbm, out_ref, h_ref, x0_ref, w1_ref, w1t_ref, w2_ref, modraw, modall, hall, sc_ref, sh_ref,
           xbuf, obuf, rbuf, robuf, gbuf, own_sem, gws, gwr, gfs, gfr, gds, gdr, ms, mr, mxs, mxr, mds, mdr, hs, hr,
           s1s, s1r, s2s, s2r, s3s, s3r, o1s, o1r, o2s, o2r, o3s, o3r):
    me_t = lax.axis_index('time')
    me_m = lax.axis_index('model')
    me_x, me_c = me_t // 2, me_t % 2
    n_g, n_x = obuf.shape[0], n_t // 2
    n_k = robuf.shape[1]
    block = xbuf.shape[2] // 2
    span = block // ROWS
    half = block // 2
    hid_dev = modraw.shape[3]
    hid = n_m * hid_dev
    chunks = [(lo, min(lo + 256, hid)) for lo in range(0, hid, 256)]
    up, down, far = (me_m + 1) % n_m, (me_m + n_m - 1) % n_m, (me_m + 2) % n_m
    mate = me_x * 2 + (me_c + 1) % 2
    lanes = ((0, up), (1, down))

    def hop(qx):
        return qx + (qx // 2) * (5 - 2 * qx)

    def peer(q, sign):
        return ((me_x + n_x + sign * hop(q // 2)) % n_x) * 2 + (me_c + q % 2) % 2

    def remote(src, dst, send, recv, **where):
        return pltpu.make_async_remote_copy(src_ref=src, dst_ref=dst, send_sem=send, recv_sem=recv, device_id=where, device_id_type=MESH_ID)

    tables = (w1t_ref, w2_ref)

    def w_rows(origin, c):
        rows = hid_dev // 2
        return pl.ds(pl.multiple_of(origin * hid_dev + c * rows, 16), rows)

    def w_first(i, d, to):
        piece = tables[i].at[w_rows(me_m, me_c)]
        return remote(piece, piece, gws.at[i, d], gwr.at[i, d], model=to)

    def w_forward(d, to):
        piece = tables[d].at[w_rows((down, up)[d], me_c)]
        return remote(piece, piece, gfs.at[d], gfr.at[d], model=to)

    def w_share(i, place):
        piece = tables[i].at[w_rows((down, up, far)[place], me_c)]
        return remote(piece, piece, gds.at[i, place], gdr.at[i, place], time=mate)

    def mod_first(i, place):
        return remote(modraw.at[i, me_m], modraw.at[i, me_m], ms.at[i, place], mr.at[i, place], model=(up, down, far)[place])

    def mod_time(qx):
        return remote(modall.at[me_t], modall.at[me_t], mxs.at[qx], mxr.at[qx], time=((me_x + hop(qx)) % n_x) * 2 + me_c)

    def mod_share(qx):
        row = ((me_x + n_x - hop(qx)) % n_x) * 2 + me_c
        return remote(modall.at[row], modall.at[row], mds.at[qx], mdr.at[qx], time=mate)

    def h_time(q):
        return remote(hall.at[me_t], hall.at[me_t], hs.at[q], hr.at[q], time=peer(q, 1))

    def x0_of(g):
        origin = (me_m + 2 * (g // 2)) % n_m
        row = (((g + 1) // 2 * n_m + origin) * n_t + me_t) * ROWS
        return x0_ref[pl.ds(pl.multiple_of(row, ROWS), ROWS), :]

    mine = pl.ds(pl.multiple_of(me_m * hid_dev, 16), hid_dev)
    own = [pltpu.make_async_copy(src, dst, own_sem.at[i]) for i, (src, dst) in enumerate((
        (ms_hbm, modraw.at[0, me_m]), (mb_hbm, modraw.at[1, me_m]), (wu_hbm, w1t_ref.at[mine]), (wd_hbm, w2_ref.at[mine]), (h_hbm, h_ref), (x0_hbm, x0_ref)))]
    for copy in own:
        copy.start()
    barrier = pltpu.get_barrier_semaphore()

    @pl.loop(1, n_t)
    def _(q):
        pl.semaphore_signal(barrier, inc=1, device_id={'time': peer(q, 1)}, device_id_type=MESH_ID)
    for to in (up, down, far):
        pl.semaphore_signal(barrier, inc=1, device_id={'model': to}, device_id_type=MESH_ID)
    for copy in own[:-1]:
        copy.wait()
    for j in range(span):
        hall[me_t, j:j + 1, :] = jnp.full((1, hall.shape[2]), h_ref[j], F32)
    pl.semaphore_wait(barrier, n_t + 2)

    for place in (2, 0, 1):
        for i in range(2):
            mod_first(i, place).start()
    for d, to in lanes:
        for i in (d, 1 - d):
            w_first(i, d, to).start()

    @pl.loop(1, n_t)
    def _(q):
        h_time(q).start()

    for place in range(3):
        for i in range(2):
            mod_first(i, place).wait_recv()
    for i in range(2):
        modall[me_t, i] = jnp.concatenate([modraw[i, m].astype(F32) for m in range(n_m)], axis=1).astype(BF16)
    for qx in (1, 2, 3):
        mod_time(qx).start()
    mod_share(0).start()
    own[-1].wait()

    @pl.loop(0, n_g * n_x)
    def _(i):
        xbuf[i // n_x, i % n_x] = jnp.concatenate([x0_of(i // n_x).astype(BF16)] * (2 * span), axis=0)

    for d, to in lanes:
        w_first(d, d, to).wait_recv()
        w_forward(d, to).start()
        w_share(d, d).start()
    for d, to in lanes:
        w_first(1 - d, d, to).wait_recv()
        w_share(1 - d, d).start()
    for qx in (1, 2, 3):
        mod_time(qx).wait_recv()
        mod_share(qx).start()
    for d, to in lanes:
        w_forward(d, to).wait_recv()
        w_share(d, 2).start()

    @pl.loop(1, n_t)
    def _(q):
        h_time(q).wait_recv()
    for qx in range(n_x):
        mod_share(qx).wait_recv()

    @pl.loop(0, n_t)
    def _(t):
        sc_ref[t] = 0.5 * (1.0 + modall[t, 0].astype(F32))
        sh_ref[t] = 0.5 * modall[t, 1].astype(F32)

    for place in range(3):
        for i in range(2):
            w_share(i, place).wait_recv()
    for lo in range(0, hid, 128):
        w1_ref[:, lo:lo + 128] = w1t_ref[lo:lo + 128, :].T

    def lift(slot, x, blocks):
        for lo, hi in chunks:
            p = jnp.dot(x, w1_ref[:, lo:hi], preferred_element_type=F32)
            for b, tb in enumerate(blocks):
                for j in range(span):
                    at = (b * span + j) * ROWS
                    v = p[at:at + ROWS] * sc_ref[tb, j:j + 1, lo:hi] + sh_ref[tb, j:j + 1, lo:hi]
                    t = jnp.tanh(v * (2 * ROOT + (8 * 0.044715 * ROOT) * (v * v)))
                    gbuf[slot, at:at + ROWS, lo:hi] = (v + v * t).astype(BF16)

    def lower(slot):
        return jnp.dot(gbuf[slot], w2_ref[...], preferred_element_type=F32)

    def scaled(f, b, tb, j):
        at = (b * span + j) * ROWS
        h = hall[tb, j:j + 1, :]
        return f[at:at + ROWS] * jnp.concatenate([h] * (f.shape[1] // h.shape[1]), axis=1)

    def place_of(g):
        return 3 * (g // 2), (g + 1) // 2

    def sweep(g, number):
        x0 = x0_of(g)
        to = g + number // (SWEEPS - 1) * (n_g - g)
        acc = jnp.zeros_like(x0)
        lift(0, xbuf[g, 0], (0, 1))
        for bx in range(n_x):
            if bx + 1 < n_x:
                lift((bx + 1) % 2, xbuf[g, bx + 1], (2 * bx + 2, 2 * bx + 3))
            f = lower(bx % 2)
            for b in range(2):
                obuf[g, 2 * bx + b] = acc
                for j in range(span):
                    at = (b * span + j) * ROWS
                    xbuf[to, bx, at:at + ROWS, :] = (x0 + acc).astype(BF16)
                    acc = acc + scaled(f, b, 2 * bx + b, j)

    def sub(c):
        return pl.ds(c * block, block)

    def x_copy(g, q, to, src):
        rel, k = place_of(g)
        return remote(xbuf.at[g, to // 2, sub(to % 2)], rbuf.at[rel, k, src // 2, sub(src % 2)], s1s.at[g, q], s1r.at[g, q], time=to)

    def x_send(g):
        @pl.loop(1, n_t)
        def _(q):
            x_copy(g, q, peer(q, 1), me_t).start()
        rel, k = place_of(g)
        rbuf[rel, k, me_x, sub(me_c), :] = xbuf[g, me_x, sub(me_c), :]

    def x_come(g, q):
        @pl.when(q > 0)
        def _():
            x_copy(g, q, me_t, peer(q, -1)).wait_recv()

    def x_ring(q, k, d, to):
        src = peer(q, -1)
        i = k * n_t + q
        return remote(rbuf.at[0, k, src // 2, sub(src % 2)], rbuf.at[1 + d, k, src // 2, sub(src % 2)], s2s.at[d, i], s2r.at[d, i], model=to)

    def x_next(q, k, d, to):
        src = peer(q, -1)
        i = k * n_t + q
        part = pl.ds((src % 2) * block + d * half, half)
        return remote(rbuf.at[1 + d, k, src // 2, part], rbuf.at[3, k, src // 2, part], s3s.at[d, i], s3r.at[d, i], model=to)

    def x_row(q, k):
        x_come(k, q)
        for d, to in lanes:
            x_ring(q, k, d, to).start()

    def x_pass(q, k):
        for d, to in lanes:
            x_ring(q, k, d, to).wait_recv()
            x_next(q, k, d, to).start()

    def x_far(q, k):
        for d, to in lanes:
            x_next(q, k, d, to).wait_recv()

    def o_copy(g, q, to, src):
        rel, k = place_of(g)
        return remote(obuf.at[g, to], robuf.at[rel, k, src], o1s.at[g, q], o1r.at[g, q], time=to)

    def o_ring(k, d, to):
        return remote(robuf.at[0, k], robuf.at[1 + d, k], o2s.at[d, k], o2r.at[d, k], model=to)

    def o_next(k, d, to):
        part = pl.ds(d * n_x, n_x)
        return remote(robuf.at[1 + d, k, part], robuf.at[3, k, part], o3s.at[d, k], o3r.at[d, k], model=to)

    def o_send(g):
        @pl.loop(1, n_t)
        def _(q):
            o_copy(g, q, peer(q, 1), me_t).start()
        rel, k = place_of(g)
        robuf[rel, k, me_t] = obuf[g, me_t]

    def o_come(g):
        @pl.loop(1, n_t)
        def _(q):
            o_copy(g, q, me_t, peer(q, -1)).wait_recv()

    def o_row(k):
        o_come(k)
        for d, to in lanes:
            o_ring(k, d, to).start()

    def o_pass(k):
        for d, to in lanes:
            o_ring(k, d, to).wait_recv()
            o_next(k, d, to).start()

    def o_far(k):
        for d, to in lanes:
            o_next(k, d, to).wait_recv()

    def finish(rels, pair):
        k, src = pair // n_x, (me_x + n_x - hop(pair % n_x)) % n_x
        for slot, rel in enumerate(rels):
            lift(slot, rbuf[rel, k, src], (me_t, me_t))
            origin = (me_m + (n_m - rel) + (rel // 2) * (2 * rel - 5)) % n_m
            row = pl.multiple_of((((k * n_m + origin) * n_x + src) * 2) * ROWS, 2 * ROWS)
            f = lower(slot)
            for b in range(2):
                x0 = x0_ref[pl.ds(row + b * ROWS, ROWS), :]
                acc = robuf[rel, k, 2 * src + b]
                for j in range(span):
                    out_ref[j, pl.ds(row + b * ROWS, ROWS), :] = x0 + acc
                    acc = acc + scaled(f, b, me_t, j)

    def row_at(i):
        x_row(i % n_t, i // n_t)

    @pl.loop(0, n_g * SWEEPS - 1)
    def _(step):
        g, number = step // SWEEPS, step % SWEEPS
        sweep(g, number)

        @pl.when(number == SWEEPS - 2)
        def _():
            x_send(g)

        @pl.when(number == SWEEPS - 1)
        def _():
            o_send(g)

        @pl.when(step == 2)
        def _():
            row_at(0)

        @pl.when(step == 3)
        def _():
            row_at(1)

        @pl.when(step == 4)
        def _():
            row_at(2)

        @pl.when(step > 3)
        def _():
            row_at(step - 1)

        @pl.when(step > 4)
        def _():
            x_pass(step - 5, 0)

        @pl.when(step == 5)
        def _():
            o_row(0)

        @pl.when(step == 7)
        def _():
            o_pass(0)

        @pl.when(step == 9)
        def _():
            o_row(1)

    passed, rowed = n_g * SWEEPS - 6, n_g * SWEEPS - 2
    o_far(0)
    for q in range(passed, n_t - 1):
        x_pass(q, 0)

    @pl.loop(0, n_k * n_x * 2)
    def _(i):
        pair, part = i // 2, i % 2
        k, at = pair // n_x, pair % n_x * 2

        @pl.when(part == 0)
        def _():
            @pl.when(pair + rowed < n_k * n_t)
            def _():
                row_at(pair + rowed)

            @pl.when(pair == 1)
            def _():
                o_pass(1)

            @pl.when(pair == n_x)
            def _():
                o_far(1)

            @pl.when(k == 1)
            def _():
                for c in range(2):
                    x_ring(at + c, 1, 0, up).wait_recv()

        @pl.when(part == 1)
        def _():
            @pl.when(pair == 0)
            def _():
                x_pass(n_t - 1, 0)

            @pl.when(k == 0)
            def _():
                for c in range(2):
                    x_far(at + c, 0)

            @pl.when(k == 1)
            def _():
                for c in range(2):
                    x_ring(at + c, 1, 1, down).wait_recv()
                    x_come(2, at + c)
        finish((2 * part, 2 * part + 1), pair)

    for d, to in lanes:
        for i in range(2):
            w_first(i, d, to).wait_send()
        w_forward(d, to).wait_send()
    for place in range(3):
        for i in range(2):
            w_share(i, place).wait_send()
            mod_first(i, place).wait_send()
    for qx in range(n_x):
        if qx:
            mod_time(qx).wait_send()
        mod_share(qx).wait_send()

    @pl.loop(1, n_t)
    def _(q):
        h_time(q).wait_send()

    @pl.loop(0, n_g * n_t)
    def _(i):
        g, q = i // n_t, i % n_t

        @pl.when(q > 0)
        def _():
            x_copy(g, q, peer(q, 1), me_t).wait_send()

            @pl.when(g < n_k)
            def _():
                o_copy(g, q, peer(q, 1), me_t).wait_send()

    @pl.loop(0, n_k * n_t)
    def _(i):
        for d, to in lanes:
            x_ring(i % n_t, i // n_t, d, to).wait_send()

    @pl.loop(0, n_t)
    def _(q):
        for d, to in lanes:
            x_next(q, 0, d, to).wait_send()
    for d, to in lanes:
        for k in range(n_k):
            o_ring(k, d, to).wait_send()
            o_next(k, d, to).wait_send()


def drain(n, src_ref, out_ref, sems):
    size = out_ref.shape[0] // n
    copies = [pltpu.make_async_copy(src_ref.at[pl.ds(i * size, size)], out_ref.at[pl.ds(i * size, size)], sems.at[i]) for i in range(n)]
    for copy in copies:
        copy.start()
    for copy in copies:
        copy.wait()


def solution(mesh):
    n_t, n_m = mesh.shape['time'], mesh.shape['model']

    def device_body(x_init, w_up, w_down, mod_scale, mod_shift, step_size):
        (span, hid_dev), chan = mod_scale.shape, x_init.shape[-1]
        rows = x_init.shape[0] * x_init.shape[1]
        hid = n_m * hid_dev
        n_k, n_x = rows // (n_t * n_m * ROWS), n_t // 2
        n_g = n_k + 1
        vmem = pl.BlockSpec(memory_space=pltpu.VMEM)
        sem = lambda *shape: pltpu.SemaphoreType.DMA(shape)
        hbm = pl.BlockSpec(memory_space=pltpu.HBM)
        out = pl.pallas_call(
            functools.partial(kernel, n_t, n_m),
            out_shape=pltpu.VMEM((span, rows, chan), F32),
            in_specs=[hbm] * 6,
            out_specs=vmem,
            scratch_shapes=[
                pltpu.SMEM((span,), F32),
                pltpu.VMEM((rows, chan), F32),
                pltpu.VMEM((chan, hid), BF16),
                pltpu.VMEM((hid, chan), BF16),
                pltpu.VMEM((hid, chan), BF16),
                pltpu.VMEM((2, n_m, span, hid_dev), BF16),
                pltpu.VMEM((n_t, 2, span, hid), BF16),
                pltpu.VMEM((n_t, span, 128), F32),
                pltpu.VMEM((n_t, span, hid), F32),
                pltpu.VMEM((n_t, span, hid), F32),
                pltpu.VMEM((n_g + 1, n_x, 2 * span * ROWS, chan), BF16),
                pltpu.VMEM((n_g, n_t, ROWS, chan), F32),
                pltpu.VMEM((n_m, n_k, n_x, 2 * span * ROWS, chan), BF16),
                pltpu.VMEM((n_m, n_k, n_t, ROWS, chan), F32),
                pltpu.VMEM((2, 2 * span * ROWS, hid), BF16),
                sem(6),
                sem(2, 2), sem(2, 2), sem(2), sem(2), sem(2, 3), sem(2, 3),
                sem(2, 3), sem(2, 3), sem(n_x), sem(n_x), sem(n_x), sem(n_x), sem(n_t), sem(n_t),
                sem(n_g, n_t), sem(n_g, n_t),
                sem(2, n_k * n_t), sem(2, n_k * n_t), sem(2, n_t), sem(2, n_t),
                sem(n_g, n_t), sem(n_g, n_t),
                sem(2, n_k), sem(2, n_k), sem(2, n_k), sem(2, n_k),
            ],
            compiler_params=pltpu.CompilerParams(collective_id=0, has_side_effects=True, vmem_limit_bytes=VMEM_BYTES - 4 * span * rows * chan),
        )(step_size, x_init.reshape(rows, chan), w_up.T, w_down, mod_scale, mod_shift)
        out = pl.pallas_call(
            functools.partial(drain, STAGES),
            out_shape=jax.ShapeDtypeStruct((span, rows, chan), F32),
            in_specs=[vmem],
            out_specs=hbm,
            scratch_shapes=[sem(STAGES)],
            compiler_params=pltpu.CompilerParams(vmem_limit_bytes=2 << 20),
        )(out)
        return out.reshape((span,) + x_init.shape)

    return jax.shard_map(device_body, mesh=mesh, in_specs=(P('data', None, None), P(None, 'model'), P('model', None), P('time', 'model'), P('time', 'model'), P('time')), out_specs=P('time', 'data', None, None), check_vma=False)
```
